256 devices in a mesh: dp: 8 (over z_lo, y), expert: 32 (over x, z_hi, core).
Axes of the slice: x: 4, y: 4, z: 8 (z_hi: 4, z_lo: 2; z = z_hi * 2 + z_lo), core: 2. Of those that a mesh axis runs over, the one named last changes fastest.
Arguments:
- tokens: bfloat16 [32768, 2048], P(('dp', 'expert')), may hold values from -6 to 6
- out_grad: bfloat16 [32768, 2048], P(('dp', 'expert')), may hold values from -6 to 6
- expert_ids: int32 [32768, 2], P(('dp', 'expert')), may hold values from 0 to 31, all different within a row; in each aligned block of 128 rows (0 to 127, 128 to 255, ...) at most 16 rows name the same one
- gate_probs: float32 [32768, 2], P(('dp', 'expert')), may hold values from 0.1 to 1
- held_expert: int32 [32], replicated, may hold values from 0 to 31, each once
- swap_pairs: int32 [4], replicated, may hold values from 0 to 15, as said below
- w_in: bfloat16 [32, 2048, 1536], P('expert', 'dp'), may hold values from -0.125 to 0.125
- w_down: bfloat16 [32, 2048, 768], P('expert', 'dp'), may hold values from -0.21875 to 0.21875
- m_in: bfloat16 [32, 2048, 1536], P('expert', 'dp'), may hold values from -12 to 12
- m_down: bfloat16 [32, 2048, 768], P('expert', 'dp'), may hold values from -12 to 12
- v_in: bfloat16 [32, 2048, 1536], P('expert', 'dp'), may hold values from 4 to 400
- v_down: bfloat16 [32, 2048, 768], P('expert', 'dp'), may hold values from 4 to 400
Outputs:
- token_grad: bfloat16 [32768, 2048], P(('dp', 'expert'))
- prob_grad: float32 [32768, 2], P(('dp', 'expert'))
- new_w_in: bfloat16 [32, 2048, 1536], P('expert', 'dp')
- new_w_down: bfloat16 [32, 2048, 768], P('expert', 'dp')
- new_m_in: bfloat16 [32, 2048, 1536], P('expert', 'dp')
- new_m_down: bfloat16 [32, 2048, 768], P('expert', 'dp')
- new_v_in: bfloat16 [32, 2048, 1536], P('expert', 'dp')
- new_v_down: bfloat16 [32, 2048, 768], P('expert', 'dp')
The draws below stay inside these ranges and needn't reach their ends.
Inputs may be any that keep to these rules, and one draw needn't show every extreme that they name: `expert_ids`: each row names 2 different experts; among the 128 rows of one device no expert is named by more than 16 rows, and some expert reaches 16. `held_expert`: A permutation of the experts. `swap_pairs`: 4 different values; value p stands for the slots p and p + 16.
All inputs are finite; a program needn't handle non-finite values.
Results may differ from the reference program's by a relative error of at most 0.02.
Values may be sent and summed in bfloat16 or wider, within the bound.
A program may use at most 128 MiB of HBM per device.

```python
import math
import jax
import jax.numpy as jnp
import numpy as np
from jax import lax

D = 2048
H = 768
TOP = 2
PAIRS = 4
TOK_DEV = 128
EXPERTS = 32
CAP = 16
TOKENS = 32768
N_DP = 8


def draw_swap_pairs(key, part):
    half_count = EXPERTS // 2
    middle = jax.random.permutation(jax.random.fold_in(key, 7), half_count - 2) + 1
    chosen = jnp.concatenate([jnp.array([0, half_count - 1], jnp.int32), middle[:PAIRS - 2].astype(jnp.int32)])
    return jax.random.permutation(jax.random.fold_in(key, 11), chosen).astype(jnp.int32)


def level_of(rng, extent, shards, smallest, top_value):
    def one(axis_at, blocks):
        heights = jax.random.uniform(jax.random.fold_in(jax.random.fold_in(rng, 6), axis_at), (blocks,), jnp.float32, smallest / len(shards), top_value / len(shards))
        return jnp.repeat(jnp.exp(heights), extent[axis_at] // blocks).reshape((-1,) + (1,) * (len(extent) - axis_at - 1))

    factor_of = one(*shards[0])
    for cut in shards[1:]:
        factor_of = factor_of * one(*cut)
    return factor_of


def routed_block(own_key, own, number, rows, amount, top, bound, lean):
    sequence = jax.random.permutation(own_key, amount)
    crowded, usual = shares(amount, rows * top, bound, lean, True), shares(amount, rows * top, bound, lean, False)
    places = jnp.arange(amount)

    def named(lengths, rotation):
        used = int((lengths > 0).sum())
        fixed = max(1, used // 4)
        passed = fixed + (places - fixed + rotation * (used - fixed)) % max(1, amount - fixed)
        return jnp.zeros((amount,), jnp.int32).at[sequence[jnp.where(places < fixed, places, passed)]].set(jnp.asarray(lengths, jnp.int32))

    lengths = jnp.where(number % 4 == 0, named(crowded, number // 4), named(usual, number - number // 4 - 1))
    mixed = jax.random.permutation(jax.random.fold_in(own, 3), amount)
    donor, sink = mixed[0:amount // 2 * 2:2], mixed[1:amount // 2 * 2:2]
    margin = jnp.minimum(lengths[donor] - 1, bound - lengths[sink]) // 2
    margin = jnp.where((donor == sequence[0]) | (sink == sequence[0]) | (lengths[sink] == 0), 0, jnp.maximum(margin, 0))
    passed = jax.random.randint(jax.random.fold_in(own, 4), (amount // 2,), 0, 1 << 20) % (margin + 1)
    lengths = lengths.at[donor].add(-passed).at[sink].add(passed)
    items = jnp.searchsorted(jnp.cumsum(lengths), jnp.arange(rows * top), side="right").astype(jnp.int32)
    grid = items.reshape(top, rows).T
    grid = grid[jax.random.permutation(jax.random.fold_in(own, 1), rows)]
    rotation = jax.random.randint(jax.random.fold_in(own, 2), (rows, 1), 0, top)
    return jnp.take_along_axis(grid, (jnp.arange(top)[None, :] + rotation) % top, axis=1)


def shares(number_of, total, most, slope, full):
    loads = [(1 << 20) // math.isqrt(rank ** slope) + 1 for rank in range(1, number_of + 1)]
    largest = most if full else min(most, max(-(-total // number_of), total * loads[0] // sum(loads)))
    least = 1 if total - largest >= number_of - 1 else 0
    given, rest = [largest] + [least] * (number_of - 1), total - largest - least * (number_of - 1)
    while rest > 0:
        movable = [i for i in range(1, number_of) if given[i] < largest] or [i for i in range(1, number_of) if given[i] < most]
        whole, remaining = sum([loads[i] for i in movable]), rest
        for i in movable:
            addition = min(most - given[i], max(1, remaining * loads[i] // whole), rest)
            given[i] = given[i] + addition
            rest = rest - addition
    return np.array(given)


def centred(rng, dims, deviation, most, pieces=(), held_as=jnp.bfloat16):
    values = jax.random.normal(rng, dims, jnp.float32) * deviation
    if len(pieces) > 0:
        values = level_of(rng, dims, pieces, -0.22, 0.18) * values
    return jnp.clip(values, min=-most, max=most).astype(held_as)


def setup_inputs(seed: int = 0) -> dict:
    seeds = jax.random.split(jax.random.key(seed), 13)
    tokens = centred(seeds[0], (TOKENS, D), 1.0, 6.0, ((0, 256),))
    out_grad = centred(seeds[1], (TOKENS, D), 1.0, 6.0, ((0, 256),))
    expert_ids_keys = jax.random.split(jax.random.fold_in(seeds[2], 1), TOKENS // TOK_DEV)
    expert_ids_turns = jax.random.permutation(jax.random.fold_in(seeds[2], 3), TOKENS // TOK_DEV)
    expert_ids = jax.vmap(lambda own, number: routed_block(jax.random.fold_in(seeds[2], 2), own, number, TOK_DEV, EXPERTS, TOP, CAP, 2))(expert_ids_keys, expert_ids_turns).reshape((TOKENS, TOP))
    gate_probs = jnp.clip(0.1 + 0.9 * jax.random.uniform(seeds[3], (TOKENS, TOP), jnp.float32) ** level_of(seeds[3], (TOKENS, TOP), ((0, 256),), -0.2, 0.2), 0.1, 1.0)
    held_expert = jax.random.permutation(seeds[4], EXPERTS).astype(jnp.int32)
    swap_pairs = draw_swap_pairs(jax.random.fold_in(seeds[12], 71), 0)
    w_in = centred(seeds[6], (EXPERTS, D, 2 * H), D ** -0.5, 0.125, ((0, 32), (1, 8)))
    w_down = centred(seeds[7], (EXPERTS, D, H), H ** -0.5, 0.21875, ((0, 32), (1, 8)))
    m_in = centred(seeds[8], (EXPERTS, D, 2 * H), 2.0, 12.0, ((0, 32), (1, 8)))
    m_down = centred(seeds[9], (EXPERTS, D, H), 2.0, 12.0, ((0, 32), (1, 8)))
    v_in = jnp.clip(jnp.exp(math.log(400.0) - 4.6051702 * jax.random.uniform(seeds[10], (EXPERTS, D, 2 * H), jnp.float32) ** level_of(seeds[10], (EXPERTS, D, 2 * H), ((0, 32), (1, 8)), -0.2, 0.2)), 4.0, 400.0).astype(jnp.bfloat16)
    v_down = jnp.clip(jnp.exp(math.log(400.0) - 4.6051702 * jax.random.uniform(seeds[11], (EXPERTS, D, H), jnp.float32) ** level_of(seeds[11], (EXPERTS, D, H), ((0, 32), (1, 8)), -0.2, 0.2)), 4.0, 400.0).astype(jnp.bfloat16)
    return dict(tokens=tokens, out_grad=out_grad, expert_ids=expert_ids, gate_probs=gate_probs, held_expert=held_expert, swap_pairs=swap_pairs, w_in=w_in, w_down=w_down, m_in=m_in, m_down=m_down, v_in=v_in, v_down=v_down)


beta_one = 0.9
beta_two = 0.95
learn_rate = 0.01
adam_eps = 1e-08
bias_one = 1.0 - 0.9 ** 10
bias_two = 1.0 - 0.95 ** 10

def expert_pass(rows_x, rows_s, weight_in, weight_down):
    half_width = weight_down.shape[1]
    projected = jnp.dot(rows_x, weight_in, preferred_element_type=jnp.float32)
    gate_part = projected[:, :half_width]
    up_part = projected[:, half_width:]
    sigmoid = jax.nn.sigmoid(gate_part)
    activated = gate_part * sigmoid
    slope_term = sigmoid * (1.0 + gate_part * (1.0 - sigmoid))
    hidden = (activated * up_part).astype(jnp.bfloat16)
    expert_out = lax.dot_general(hidden, weight_down, (((1,), (1,)), ((), ())), preferred_element_type=jnp.float32).astype(jnp.bfloat16)
    hidden_grad = jnp.dot(rows_s, weight_down, preferred_element_type=jnp.float32)
    pre_grad = jnp.concatenate([hidden_grad * up_part * slope_term, hidden_grad * activated], axis=1).astype(jnp.bfloat16)
    row_grad = lax.dot_general(pre_grad, weight_in, (((1,), (1,)), ((), ())), preferred_element_type=jnp.float32).astype(jnp.bfloat16)
    grad_in = lax.dot_general(rows_x, pre_grad, (((0,), (0,)), ((), ())), preferred_element_type=jnp.float32).astype(jnp.bfloat16)
    grad_down = lax.dot_general(rows_s, hidden, (((0,), (0,)), ((), ())), preferred_element_type=jnp.float32).astype(jnp.bfloat16)
    return (row_grad, expert_out, grad_in, grad_down)

def adam_update(weight, first, second, grad):
    first_new = beta_one * first.astype(jnp.float32) + (1.0 - beta_one) * grad
    second_new = beta_two * second.astype(jnp.float32) + (1.0 - beta_two) * grad * grad
    step_size = first_new / bias_one / (jnp.sqrt(second_new / bias_two) + adam_eps)
    weight_new = weight.astype(jnp.float32) - learn_rate * step_size
    return (weight_new.astype(jnp.bfloat16), first_new.astype(jnp.bfloat16), second_new.astype(jnp.bfloat16))

def swap_slots(array, swap_flag):
    partner = jnp.roll(array, EXPERTS // 2, axis=0)
    flag_shape = swap_flag.reshape((-1,) + (1,) * (array.ndim - 1))
    return jnp.where(flag_shape, partner, array)

def reference(tokens, out_grad, expert_ids, gate_probs, held_expert, swap_pairs, w_in, w_down, m_in, m_down, v_in, v_down):
    half_count = EXPERTS // 2
    slot_ids = jnp.arange(EXPERTS, dtype=jnp.int32)
    swap_flag = jnp.any((slot_ids % half_count)[:, None] == swap_pairs[None, :], axis=1)
    held_after = swap_slots(held_expert, swap_flag)
    state_in = swap_slots(w_in, swap_flag)
    state_down = swap_slots(w_down, swap_flag)
    first_in = swap_slots(m_in, swap_flag)
    first_down = swap_slots(m_down, swap_flag)
    second_in = swap_slots(v_in, swap_flag)
    second_down = swap_slots(v_down, swap_flag)
    group_tokens = EXPERTS * TOK_DEV
    picks = group_tokens * TOP
    room = EXPERTS * CAP
    scaled = (gate_probs[:, :, None] * out_grad[:, None, :].astype(jnp.float32)).astype(jnp.bfloat16)
    tokens_grouped = tokens.reshape(N_DP, group_tokens, D)
    scaled_grouped = scaled.reshape(N_DP, picks, D)
    ids_grouped = expert_ids.reshape(N_DP, picks)

    def one_group(expert, weight_in, weight_down, group_x, group_s, group_ids):
        hits = group_ids == expert
        found = jnp.nonzero(hits, size=room, fill_value=0)[0].astype(jnp.int32)
        valid = jnp.arange(room, dtype=jnp.int32) < jnp.sum(hits.astype(jnp.int32))
        rows_x = jnp.where(valid[:, None], group_x[found // TOP], jnp.zeros((), jnp.bfloat16))
        rows_s = jnp.where(valid[:, None], group_s[found], jnp.zeros((), jnp.bfloat16))
        row_grad, expert_out, grad_in, grad_down = expert_pass(rows_x, rows_s, weight_in, weight_down)
        target = jnp.where(valid, found, picks).astype(jnp.int32)
        return (row_grad, expert_out, target, grad_in, grad_down)

    def one_slot(packed):
        expert, weight_in, weight_down = packed

        def per_group(group):
            return one_group(expert, weight_in, weight_down, group[0], group[1], group[2])
        row_grad, expert_out, target, grad_in, grad_down = lax.map(per_group, (tokens_grouped, scaled_grouped, ids_grouped))
        return (row_grad, expert_out, target, lax.optimization_barrier(jnp.sum(grad_in.astype(jnp.float32), axis=0)), lax.optimization_barrier(jnp.sum(grad_down.astype(jnp.float32), axis=0)))
    row_grad, expert_out, target, grad_in, grad_down = lax.map(one_slot, (held_after, state_in, state_down))

    def place(values, where_to):
        flat_pos = where_to.reshape(-1)
        flat_values = values.reshape((flat_pos.shape[0],) + values.shape[2:])
        base = jnp.zeros((picks,) + values.shape[2:], values.dtype)
        return base.at[flat_pos].set(flat_values, mode='drop')
    grads_picked = jax.vmap(place, in_axes=(1, 1))(row_grad, target)
    outs_picked = jax.vmap(place, in_axes=(1, 1))(expert_out, target)
    token_grad = lax.optimization_barrier(jnp.sum(grads_picked.reshape(N_DP, group_tokens, TOP, D).astype(jnp.float32), axis=2)).astype(jnp.bfloat16).reshape(TOKENS, D)
    prob_grad = lax.optimization_barrier(jnp.sum(outs_picked.reshape(TOKENS, TOP, D).astype(jnp.float32) * out_grad[:, None, :].astype(jnp.float32), axis=2))
    new_w_in, new_m_in, new_v_in = adam_update(state_in, first_in, second_in, grad_in)
    new_w_down, new_m_down, new_v_down = adam_update(state_down, first_down, second_down, grad_down)
    return (token_grad, prob_grad, new_w_in, new_w_down, new_m_in, new_m_down, new_v_in, new_v_down)
```

```python
import functools

import jax
import jax.numpy as jnp
from jax import lax
from jax.experimental import pallas as pl
from jax.experimental.pallas import tpu as pltpu
from jax.sharding import Mesh
from jax.sharding import PartitionSpec as P

DP = ("dp_0", "dp_1")
DP_EXPERT = ("dp_0", "dp_1", "expert")
MESH = pl.DeviceIdType.MESH
BF16, F32 = jnp.bfloat16, jnp.float32

beta_one = 0.9
beta_two = 0.95
learn_rate = 0.01
adam_eps = 1e-08
bias_one = 1.0 - 0.9**10
bias_two = 1.0 - 0.95**10

LANES = 128
GATHER_CHUNKS = 2
SUM_CHUNKS = 4
EARLY_SENDS = 10
VMEM_BYTES = 60 * 1024 * 1024


def in_parts(column):
    high = column.astype(BF16).astype(F32)
    rest = column - high
    middle = rest.astype(BF16).astype(F32)
    low = rest - middle
    lane = lax.broadcasted_iota(jnp.int32, (column.shape[0], LANES), 1)
    low = jnp.where(lane == 2, low, 0.0)
    return jnp.where(lane == 0, high, jnp.where(lane == 1, middle, low)).astype(BF16)


def from_parts(parts):
    parts = parts.astype(F32)
    return parts[:, 0:1] + parts[:, 1:2] + parts[:, 2:3]


def dot(a, b, contract=(1, 0)):
    dims = (((contract[0],), (contract[1],)), ((), ()))
    return lax.dot_general(a, b, dims, preferred_element_type=F32)


def swapped_here(pairs_ref, me, half_axis):
    mine = lax.rem(me, half_axis)
    flag = (mine == pairs_ref[0]).astype(jnp.int32)
    for j in range(1, pairs_ref.shape[0]):
        flag = jnp.maximum(flag, (mine == pairs_ref[j]).astype(jnp.int32))
    return flag


def choose(flag, moved, kept):
    return jnp.where(jnp.full(kept.shape, flag, jnp.int32) > 0, moved.astype(F32), kept.astype(F32))


def send(source, target, sems, at, device):
    return pltpu.make_async_remote_copy(
        src_ref=source,
        dst_ref=target,
        send_sem=sems[0].at[at],
        recv_sem=sems[1].at[at],
        device_id=device,
        device_id_type=MESH,
    )


class Place:
    def __init__(self):
        self.z, self.y = lax.axis_index("dp_0"), lax.axis_index("dp_1")
        self.me = lax.axis_index("expert")
        self.layers, self.ring = lax.axis_size("dp_0"), lax.axis_size("dp_1")
        self.experts = lax.axis_size("expert")
        self.across = {"dp_0": 1 - self.z}
        self.up = {"dp_1": lax.rem(self.y + 1, self.ring)}
        self.down = {"dp_1": lax.rem(self.y + self.ring - 1, self.ring)}

    def later(self, k):
        return {"expert": lax.rem(self.me + k, self.experts)}

    def offset(self, i):
        return (i % 2) * ((i + 1) // 2) + (1 - i % 2) * (self.experts - i // 2)

    def shard(self, layer, step):
        z = (self.z + layer) % self.layers
        return z * self.ring + (self.y + step) % self.ring

    def greet(self):
        barrier = pltpu.get_barrier_semaphore()

        def hello(k, carry):
            pl.semaphore_signal(barrier, inc=1, device_id=self.later(k), device_id_type=MESH)
            return carry

        lax.fori_loop(1, self.experts, hello, 0)
        for device in (self.across, self.up, self.down):
            pl.semaphore_signal(barrier, inc=1, device_id=device, device_id_type=MESH)
        pl.semaphore_wait(barrier, self.experts - 1 + 3)


def gather_kernel(
    ids_ref, held_ref, pairs_ref, probs_ref, tokens_ref, grads_ref, w_in_ref, w_down_ref,
    recv_ref, full_ref, hots_ref,
    send_ref, swap_in, swap_down, row_send, row_recv, swap_send, swap_recv, ring_send, ring_recv,
):
    at = Place()
    experts, half_axis = at.experts, at.experts // 2
    tok_rows, width = tokens_ref.shape
    room = send_ref.shape[0]
    capacity = room // experts
    wide = w_in_ref.shape[1]
    depth = w_in_ref.shape[0]
    part = depth // GATHER_CHUNKS
    at.greet()

    partner = at.later(half_axis)
    sems = (swap_send, swap_recv)
    swaps = []
    for c in range(GATHER_CHUNKS):
        rows = pl.ds(c * part, part)
        swaps.append(
            (
                send(w_in_ref.at[rows], swap_in.at[rows], sems, (0, c), partner),
                send(w_down_ref.at[rows], swap_down.at[rows], sems, (1, c), partner),
            )
        )
        for copy in swaps[-1]:
            copy.start()

    slot = lax.broadcasted_iota(jnp.int32, (experts, 1), 0)
    flag = (slot % half_axis == pairs_ref[0]).astype(jnp.int32)
    for j in range(1, pairs_ref.shape[0]):
        flag = jnp.maximum(flag, (slot % half_axis == pairs_ref[j]).astype(jnp.int32))
    held = jnp.where(flag > 0, held_ref[:, 1:2], held_ref[:, 0:1])
    hits = [(ids_ref[k : k + 1, :] == held).astype(F32) for k in range(ids_ref.shape[0])]
    named = hits[0]
    for hit in hits[1:]:
        named = named + hit
    row = lax.broadcasted_iota(jnp.int32, (tok_rows, tok_rows), 0)
    column = lax.broadcasted_iota(jnp.int32, (tok_rows, tok_rows), 1)
    before = dot(named.astype(BF16), (row < column).astype(F32).astype(BF16))
    first = (((slot + experts - at.me) % experts) * capacity).astype(F32)
    room_ids = lax.broadcasted_iota(jnp.int32, (room, tok_rows), 0)
    parts = jnp.zeros((room, LANES), F32)
    both = jnp.zeros((room, tok_rows), F32)
    for k, hit in enumerate(hits):
        place = jnp.sum(hit * (before + first), axis=0, keepdims=True).astype(jnp.int32)
        hot = (room_ids == place).astype(F32)
        hots_ref[k] = hot.astype(BF16)
        both = both + hot
        parts = parts + dot(hot.astype(BF16), in_parts(probs_ref[:, k : k + 1]))
    send_ref[:, 2 * width :] = parts.astype(BF16)
    both = both.astype(BF16)
    step = min(512, width)
    for c in range(width // step):
        columns = pl.ds(c * step, step)
        send_ref[:, columns] = dot(both, tokens_ref[:, columns]).astype(BF16)
        send_ref[:, pl.ds(width + c * step, step)] = dot(both, grads_ref[:, columns]).astype(BF16)

    def rows_to(i):
        k = at.offset(i)
        rows = pl.ds(k * capacity, capacity)
        copy = pltpu.make_async_remote_copy(
            src_ref=send_ref.at[rows],
            dst_ref=recv_ref.at[rows],
            send_sem=row_send.at[k],
            recv_sem=row_recv.at[k],
            device_id=at.later(k),
            device_id_type=MESH,
        )
        return copy

    def start_rows(i, carry):
        rows_to(i).start()
        return carry

    def wait_rows(i, carry):
        rows_to(i).wait()
        return carry

    early = min(EARLY_SENDS, experts - 1)
    lax.fori_loop(1, 1 + early, start_rows, 0)
    recv_ref[0:capacity] = send_ref[0:capacity]

    flag = swapped_here(pairs_ref, at.me, half_axis)
    ring = (ring_send, ring_recv)

    def shard(layer, step, c):
        start = at.shard(layer, step) * depth + c * part
        return full_ref.at[pl.ds(pl.multiple_of(start, part), part)]

    def spread(kind, layer, step, c, device):
        block = shard(layer, step, c)
        return send(block, block, ring, (kind, c), device)

    sent = []

    def begin(*what):
        copy = spread(*what)
        copy.start()
        sent.append(copy)

    ACROSS, UP_OWN, DOWN_OWN, UP_OTHER, DOWN_OTHER, UP_ON, DOWN_ON = range(7)
    for c in range(GATHER_CHUNKS):
        for copy in swaps[c]:
            copy.wait_recv()
        rows = pl.ds(c * part, part)
        mine = shard(0, 0, c)
        mine[:, pl.ds(0, wide)] = choose(flag, swap_in[rows], w_in_ref[rows]).astype(BF16)
        mine[:, pl.ds(wide, w_down_ref.shape[1])] = choose(
            flag, swap_down[rows], w_down_ref[rows]
        ).astype(BF16)
        begin(ACROSS, 0, 0, c, at.across)
        begin(UP_OWN, 0, 0, c, at.up)
        begin(DOWN_OWN, 0, 0, c, at.down)
    lax.fori_loop(1 + early, experts, start_rows, 0)
    for c in range(GATHER_CHUNKS):
        spread(UP_OWN, 0, -1, c, at.up).wait_recv()
        begin(UP_ON, 0, -1, c, at.up)
        spread(ACROSS, 1, 0, c, at.across).wait_recv()
        begin(UP_OTHER, 1, 0, c, at.up)
        begin(DOWN_OTHER, 1, 0, c, at.down)
    for c in range(GATHER_CHUNKS):
        spread(DOWN_OTHER, 1, 1, c, at.down).wait_recv()
        begin(DOWN_ON, 1, 1, c, at.down)
    lax.fori_loop(1, experts, wait_rows, 0)
    for c in range(GATHER_CHUNKS):
        spread(DOWN_OWN, 0, 1, c, at.down).wait_recv()
        spread(UP_OTHER, 1, -1, c, at.up).wait_recv()
        spread(UP_ON, 0, -2, c, at.up).wait_recv()
        spread(DOWN_ON, 1, 2, c, at.down).wait_recv()
        for copy in swaps[c]:
            copy.wait_send()
    for copy in sent:
        copy.wait_send()


def expert_kernel(
    recv_ref, full_ref, hots_ref, pairs_ref, m_in_ref, m_down_ref, v_in_ref, v_down_ref,
    token_ref, prob_ref, nw_in, nw_down, nm_in, nm_down, nv_in, nv_down,
    scaled, pre, hidden, grad, ret, back, on_up, on_down,
    a_low, a_high, b_low, b_high, z_out, z_in, pm_in, pm_down, pv_in, pv_down,
    row_send, row_recv, swap_send, swap_recv, ring_send, ring_recv,
):
    at = Place()
    experts, half_axis = at.experts, at.experts // 2
    room = recv_ref.shape[0]
    capacity = room // experts
    width = token_ref.shape[1]
    half_width = hidden.shape[1]
    wide = 2 * half_width
    depth = m_in_ref.shape[0]
    part = depth // SUM_CHUNKS
    at.greet()

    partner = at.later(half_axis)
    swaps = []
    for n, (own, other) in enumerate(
        ((m_in_ref, pm_in), (m_down_ref, pm_down), (v_in_ref, pv_in), (v_down_ref, pv_down))
    ):
        swaps.append(send(own, other, (swap_send, swap_recv), n, partner))
        swaps[-1].start()

    rows_p = from_parts(recv_ref[:, 2 * width :])
    step = min(512, width)
    for c in range(width // step):
        columns = pl.ds(c * step, step)
        rows_g = recv_ref[:, pl.ds(width + c * step, step)].astype(F32)
        scaled[:, columns] = (rows_p * rows_g).astype(BF16)
    block = min(256, half_width)

    def through(n, carry):
        gate_at = pl.multiple_of(n * block, block)
        up_at = pl.multiple_of(half_width + n * block, block)
        down_at = pl.multiple_of(wide + n * block, block)
        gate_part = dot(recv_ref[:, :width], full_ref[:, pl.ds(gate_at, block)])
        up_part = dot(recv_ref[:, :width], full_ref[:, pl.ds(up_at, block)])
        hidden_grad = dot(scaled[...], full_ref[:, pl.ds(down_at, block)])
        sigmoid = jax.nn.sigmoid(gate_part)
        activated = gate_part * sigmoid
        slope_term = sigmoid * (1.0 + gate_part * (1.0 - sigmoid))
        hidden[:, pl.ds(gate_at, block)] = (activated * up_part).astype(BF16)
        pre[:, pl.ds(gate_at, block)] = (hidden_grad * up_part * slope_term).astype(BF16)
        pre[:, pl.ds(up_at, block)] = (hidden_grad * activated).astype(BF16)
        return carry

    lax.fori_loop(0, half_width // block, through, 0)

    def weight_grads(i, carry):
        start = pl.multiple_of(at.shard(i % 2, 2 + i // 2) * depth, depth)
        columns = pl.ds(start, depth)
        grad[i, :, pl.ds(0, wide)] = dot(recv_ref[:, columns], pre[...], (0, 0)).astype(BF16)
        grad[i, :, pl.ds(wide, half_width)] = dot(
            scaled[:, columns], hidden[...], (0, 0)
        ).astype(BF16)
        return carry

    ring = (ring_send, ring_recv)
    sent = []

    def begin(source, target, kind, c, device):
        copy = send(source, target.at[c], ring, (kind, c), device)
        copy.start()
        sent.append(copy)

    def arrived(target, kind, c):
        send(target.at[c], target.at[c], ring, (kind, c), at.up).wait_recv()
        return target[c].astype(F32)

    def rows_of(c):
        return pl.ds(c * part, part)

    A2, B2, A3, B3, A0, B0, A1, B1 = range(8)
    ON_UP, ON_DOWN, A_LOW, A_HIGH, B_LOW, B_HIGH, Z = range(7)
    lax.fori_loop(0, 2, weight_grads, 0)
    for c in range(SUM_CHUNKS):
        begin(grad.at[A2, rows_of(c)], on_up, ON_UP, c, at.up)
        begin(grad.at[B2, rows_of(c)], on_down, ON_DOWN, c, at.down)
    lax.fori_loop(2, 8, weight_grads, 0)
    early = SUM_CHUNKS // 2
    for c in range(early):
        begin(grad.at[B1, rows_of(c)], b_low, B_LOW, c, at.up)
        begin(grad.at[A3, rows_of(c)], a_high, A_HIGH, c, at.down)

    block = min(256, width)

    def row_grads(n, total):
        start = pl.multiple_of(n * block, block)
        rows = pl.ds(start, block)
        ret[:, rows] = dot(pre[...], full_ref[rows, pl.ds(0, wide)], (1, 1)).astype(BF16)
        out = dot(hidden[...], full_ref[rows, pl.ds(wide, half_width)], (1, 1)).astype(BF16)
        rows_g = recv_ref[:, pl.ds(pl.multiple_of(width + start, block), block)].astype(F32)
        return total + jnp.sum(out.astype(F32) * rows_g, axis=1, keepdims=True)

    total = lax.fori_loop(0, width // block, row_grads, jnp.zeros((room, 1), F32))
    ret[:, width:] = in_parts(total)

    def rows_to(i):
        k = at.offset(i)
        rows = pl.ds(k * capacity, capacity)
        return pltpu.make_async_remote_copy(
            src_ref=ret.at[rows],
            dst_ref=back.at[rows],
            send_sem=row_send.at[k],
            recv_sem=row_recv.at[k],
            device_id=at.later(experts - k),
            device_id_type=MESH,
        )

    def start_rows(i, carry):
        rows_to(i).start()
        return carry

    def wait_rows(i, carry):
        rows_to(i).wait()
        return carry

    lax.fori_loop(1, experts, start_rows, 0)
    back[0:capacity] = ret[0:capacity]

    def pass_on(c):
        low = grad[A1, rows_of(c)].astype(F32) + arrived(on_up, ON_UP, c)
        grad[A1, rows_of(c)] = low.astype(BF16)
        begin(grad.at[A1, rows_of(c)], a_low, A_LOW, c, at.up)
        high = grad[B3, rows_of(c)].astype(F32) + arrived(on_down, ON_DOWN, c)
        grad[B3, rows_of(c)] = high.astype(BF16)
        begin(grad.at[B3, rows_of(c)], b_high, B_HIGH, c, at.down)

    for c in range(SUM_CHUNKS):
        pass_on(c)
        if c + early < SUM_CHUNKS:
            begin(grad.at[B1, rows_of(c + early)], b_low, B_LOW, c + early, at.up)
            begin(grad.at[A3, rows_of(c + early)], a_high, A_HIGH, c + early, at.down)

    def hand_over(c):
        mine = grad[B0, rows_of(c)].astype(F32)
        mine = mine + arrived(b_low, B_LOW, c) + arrived(b_high, B_HIGH, c)
        z_out[c] = mine.astype(BF16)
        begin(z_out.at[c], z_in, Z, c, at.across)

    flag = swapped_here(pairs_ref, at.me, half_axis)

    def adam(c):
        rows = rows_of(c)
        mine = grad[A0, rows].astype(F32)
        mine = mine + arrived(a_low, A_LOW, c) + arrived(a_high, A_HIGH, c)
        mine = mine + arrived(z_in, Z, c)
        own = pl.ds(pl.multiple_of(at.shard(0, 0) * depth + c * part, part), part)
        for columns, refs in (
            (pl.ds(0, wide), (pm_in, m_in_ref, pv_in, v_in_ref, nw_in, nm_in, nv_in)),
            (
                pl.ds(wide, half_width),
                (pm_down, m_down_ref, pv_down, v_down_ref, nw_down, nm_down, nv_down),
            ),
        ):
            value = mine[:, columns.start : columns.start + columns.size]
            first = choose(flag, refs[0][rows], refs[1][rows])
            second = choose(flag, refs[2][rows], refs[3][rows])
            weight = full_ref[own, columns].astype(F32)
            first_new = beta_one * first + (1.0 - beta_one) * value
            second_new = beta_two * second + (1.0 - beta_two) * value * value
            step_size = first_new / bias_one / (jnp.sqrt(second_new / bias_two) + adam_eps)
            refs[4][rows] = (weight - learn_rate * step_size).astype(BF16)
            refs[5][rows] = first_new.astype(BF16)
            refs[6][rows] = second_new.astype(BF16)

    for c in range(early):
        hand_over(c)
    for copy in swaps:
        copy.wait()
    lax.fori_loop(1, experts, wait_rows, 0)
    hots = [hots_ref[k] for k in range(hots_ref.shape[0])]
    both = hots[0]
    for hot in hots[1:]:
        both = both + hot
    step = min(512, width)
    for c in range(width // step):
        columns = pl.ds(c * step, step)
        token_ref[:, columns] = dot(both, back[:, columns], (0, 0)).astype(BF16)
    for k, hot in enumerate(hots):
        prob_ref[:, k : k + 1] = from_parts(dot(hot, back[:, width:], (0, 0)))
    for c in range(early, SUM_CHUNKS):
        hand_over(c)
        adam(c - early)
    for c in range(SUM_CHUNKS - early, SUM_CHUNKS):
        adam(c)
    for copy in sent:
        copy.wait_send()


def body(
    tokens,
    out_grad,
    expert_ids,
    gate_probs,
    held_expert,
    swap_pairs,
    w_in,
    w_down,
    m_in,
    m_down,
    v_in,
    v_down,
):
    experts = lax.axis_size("expert")
    dp = lax.axis_size(DP)
    tok_rows, width = tokens.shape
    top_count = expert_ids.shape[1]
    capacity = max(2, 2 * tok_rows * top_count // experts)
    room = experts * capacity
    _, depth, wide = w_in.shape
    half_width = w_down.shape[2]
    row_width = 2 * width + LANES
    held = jnp.stack([held_expert, jnp.roll(held_expert, experts // 2)], axis=1)
    vmem = pl.BlockSpec(memory_space=pltpu.VMEM)
    smem = pl.BlockSpec(memory_space=pltpu.SMEM)
    dma = pltpu.SemaphoreType.DMA
    shape = jax.ShapeDtypeStruct
    part = depth // GATHER_CHUNKS
    recv, full, hots = pl.pallas_call(
        gather_kernel,
        name="gather",
        out_shape=(
            shape((room, row_width), BF16),
            shape((dp * depth, wide + half_width), BF16),
            shape((top_count, room, tok_rows), BF16),
        ),
        in_specs=[vmem, vmem, smem, vmem, vmem, vmem, vmem, vmem],
        out_specs=(vmem,) * 3,
        scratch_shapes=[
            pltpu.VMEM((room, row_width), BF16),
            pltpu.VMEM((depth, wide), BF16),
            pltpu.VMEM((depth, half_width), BF16),
            dma((experts,)),
            dma((experts,)),
            dma((2, GATHER_CHUNKS)),
            dma((2, GATHER_CHUNKS)),
            dma((7, GATHER_CHUNKS)),
            dma((7, GATHER_CHUNKS)),
        ],
        compiler_params=pltpu.CompilerParams(
            collective_id=0, has_side_effects=True, vmem_limit_bytes=VMEM_BYTES
        ),
    )(expert_ids.T, held, swap_pairs, gate_probs, tokens, out_grad, w_in[0], w_down[0])
    part = depth // SUM_CHUNKS
    chunked = (SUM_CHUNKS, part, wide + half_width)
    state_in, state_down = shape((depth, wide), BF16), shape((depth, half_width), BF16)
    result = pl.pallas_call(
        expert_kernel,
        name="expert",
        out_shape=(shape((tok_rows, width), BF16), shape((tok_rows, top_count), F32))
        + (state_in, state_down) * 3,
        in_specs=[vmem, vmem, vmem, smem] + [vmem] * 4,
        out_specs=(vmem,) * 8,
        scratch_shapes=[
            pltpu.VMEM((room, width), BF16),
            pltpu.VMEM((room, wide), BF16),
            pltpu.VMEM((room, half_width), BF16),
            pltpu.VMEM((dp, depth, wide + half_width), BF16),
            pltpu.VMEM((room, width + LANES), BF16),
            pltpu.VMEM((room, width + LANES), BF16),
        ]
        + [pltpu.VMEM(chunked, BF16)] * 8
        + [pltpu.VMEM((depth, wide), BF16), pltpu.VMEM((depth, half_width), BF16)] * 2
        + [dma((experts,))] * 2
        + [dma((4,))] * 2
        + [dma((7, SUM_CHUNKS))] * 2,
        compiler_params=pltpu.CompilerParams(
            collective_id=1, has_side_effects=True, vmem_limit_bytes=VMEM_BYTES
        ),
    )(recv, full, hots, swap_pairs, m_in[0], m_down[0], v_in[0], v_down[0])
    return result[:2] + tuple(r[None] for r in result[2:])


def solution(mesh):
    split = Mesh(mesh.devices.reshape(2, 4, mesh.shape["expert"]), ("dp_0", "dp_1", "expert"))
    rows = P(DP_EXPERT, None)
    state = P("expert", DP, None)
    return jax.shard_map(
        body,
        mesh=split,
        in_specs=(rows,) * 4 + (P(), P()) + (state,) * 6,
        out_specs=(rows, rows) + (state,) * 6,
        check_vma=False,
    )
```

```python
import functools

import jax
import jax.numpy as jnp
from jax import lax
from jax.experimental import pallas as pl
from jax.experimental.pallas import tpu as pltpu
from jax.sharding import Mesh
from jax.sharding import PartitionSpec as P

DP = ("dp_0", "dp_1")
EXPERT = ("ex", "ez", "ec")
DP_EXPERT = DP + EXPERT
MESH = pl.DeviceIdType.MESH
BF16, F32 = jnp.bfloat16, jnp.float32

beta_one = 0.9
beta_two = 0.95
learn_rate = 0.01
adam_eps = 1e-08
bias_one = 1.0 - 0.9**10
bias_two = 1.0 - 0.95**10

LANES = 128
GATHER_CHUNKS = 4
SUM_CHUNKS = 4
ADAM_STEPS = 4
VMEM_BYTES = 60 * 1024 * 1024


def in_parts(column):
    high = column.astype(BF16).astype(F32)
    rest = column - high
    middle = rest.astype(BF16).astype(F32)
    return [high, middle, rest - middle]


def in_lanes(columns):
    lane = lax.broadcasted_iota(jnp.int32, (columns[0].shape[0], LANES), 1)
    result = jnp.zeros(lane.shape, F32)
    for n, column in enumerate(columns):
        result = jnp.where(lane == n, column, result)
    return result.astype(BF16)


def from_parts(parts, start=0):
    parts = parts.astype(F32)
    high, middle, low = (parts[:, start + n : start + n + 1] for n in range(3))
    return high + middle + low


def column_of(row, turn=0):
    n = row.shape[1]
    at, lane = (lax.broadcasted_iota(jnp.int32, (n, n), d) for d in (0, 1))
    return jnp.sum(jnp.where(lane == lax.rem(at + turn, n), row, 0.0), axis=1, keepdims=True)


def row_of(column):
    n = column.shape[0]
    at, lane = (lax.broadcasted_iota(jnp.int32, (n, n), d) for d in (0, 1))
    return jnp.sum(jnp.where(lane == at, column, 0.0), axis=0, keepdims=True)


def dot(a, b, contract=(1, 0)):
    dims = (((contract[0],), (contract[1],)), ((), ()))
    return lax.dot_general(a, b, dims, preferred_element_type=F32)


def swapped_here(pairs_ref, me, half_axis):
    mine = lax.rem(me, half_axis)
    flag = (mine == pairs_ref[0]).astype(jnp.int32)
    for j in range(1, pairs_ref.shape[0]):
        flag = jnp.maximum(flag, (mine == pairs_ref[j]).astype(jnp.int32))
    return flag


def choose(flag, moved, kept):
    return jnp.where(jnp.full(kept.shape, flag, jnp.int32) > 0, moved.astype(F32), kept.astype(F32))


def send(source, target, sems, at, device):
    return pltpu.make_async_remote_copy(
        src_ref=source,
        dst_ref=target,
        send_sem=sems[0].at[at],
        recv_sem=sems[1].at[at],
        device_id=device,
        device_id_type=MESH,
    )


class Place:
    def __init__(self):
        self.z, self.y = lax.axis_index("dp_0"), lax.axis_index("dp_1")
        self.layers, self.ring = lax.axis_size("dp_0"), lax.axis_size("dp_1")
        self.cores, self.planes = lax.axis_size("ec"), lax.axis_size("ez")
        self.side = lax.axis_size("ex") * self.cores
        self.experts = self.side * self.planes
        self.own = lax.axis_index("ex") * self.cores + lax.axis_index("ec")
        self.plane = lax.axis_index("ez")
        self.me = (
            lax.axis_index("ex") * self.planes + self.plane
        ) * self.cores + lax.axis_index("ec")
        self.across = {"dp_0": 1 - self.z}
        self.up = {"dp_1": lax.rem(self.y + 1, self.ring)}
        self.down = {"dp_1": lax.rem(self.y + self.ring - 1, self.ring)}

    def member(self, sideways, planes):
        q = (self.own + sideways) % self.side
        z = (self.plane + planes) % self.planes
        return {"ex": q // self.cores, "ez": z, "ec": q % self.cores}

    def partner(self):
        e = (self.me + self.experts // 2) % self.experts
        return {
            "ex": e // (self.planes * self.cores),
            "ez": (e // self.cores) % self.planes,
            "ec": e % self.cores,
        }

    def offset(self, i):
        return (i % 2) * ((i + 1) // 2) + (1 - i % 2) * (self.experts - i // 2)

    def shard(self, layer, step):
        z = (self.z + layer) % self.layers
        return z * self.ring + (self.y + step) % self.ring

    def greet(self):
        barrier = pltpu.get_barrier_semaphore()

        def hello(k, carry):
            device = self.member(k % self.side, k // self.side)
            pl.semaphore_signal(barrier, inc=1, device_id=device, device_id_type=MESH)
            return carry

        lax.fori_loop(1, self.experts, hello, 0)
        for device in (self.across, self.up, self.down):
            pl.semaphore_signal(barrier, inc=1, device_id=device, device_id_type=MESH)
        pl.semaphore_wait(barrier, self.experts - 1 + 3)


def layer_kernel(
    ids_ref, held_ref, pairs_ref, probs_ref, tokens_ref, grads_ref, w_in_ref, w_down_ref,
    m_in_ref, m_down_ref, v_in_ref, v_down_ref,
    total_ref, weight_ref, back, hots_ref, pm_in, pm_down, pv_in, pv_down,
    tok, send_ref, recv, full_ref, swap_in, swap_down, scaled, pre, hidden, grad, ret,
    on_up, on_down, a_low, a_high, b_low, b_high, z_in,
    tok_send, tok_recv, row_send, row_recv, back_send, back_recv, swap_send, swap_recv,
    moment_send, moment_recv, gather_send, gather_recv, ring_send, ring_recv,
):
    at = Place()
    experts, half_axis = at.experts, at.experts // 2
    tok_rows, width = tokens_ref.shape
    room, row_width = recv.shape
    capacity = room // experts
    plane_room = room // at.planes
    depth, wide = w_in_ref.shape
    half_width = w_down_ref.shape[1]
    at.greet()

    part = depth // GATHER_CHUNKS
    partner = at.partner()
    sems = (swap_send, swap_recv)
    swaps = []
    for c in range(GATHER_CHUNKS):
        rows = pl.ds(c * part, part)
        swaps.append(
            (
                send(w_in_ref.at[rows], swap_in.at[rows], sems, (0, c), partner),
                send(w_down_ref.at[rows], swap_down.at[rows], sems, (1, c), partner),
            )
        )
        for copy in swaps[-1]:
            copy.start()

    slot = lax.broadcasted_iota(jnp.int32, (1, experts), 1)
    flag = (lax.rem(slot, half_axis) == pairs_ref[0]).astype(jnp.int32)
    for j in range(1, pairs_ref.shape[0]):
        flag = jnp.maximum(flag, (lax.rem(slot, half_axis) == pairs_ref[j]).astype(jnp.int32))
    before_swap = held_ref[...].astype(F32)
    held = jnp.where(flag > 0, row_of(column_of(before_swap, half_axis)), before_swap)
    top_count = ids_ref.shape[0]
    hits = [
        (column_of(ids_ref[k : k + 1, :].astype(F32)) == held).astype(F32)
        for k in range(top_count)
    ]
    named = hits[0]
    for hit in hits[1:]:
        named = named + hit
    row, column = (lax.broadcasted_iota(jnp.int32, (tok_rows, tok_rows), d) for d in (0, 1))
    before = dot((column < row).astype(F32).astype(BF16), named.astype(BF16))
    in_plane = lax.div(slot, at.planes * at.cores) * at.cores + lax.rem(slot, at.cores)
    planes_on = lax.rem(lax.rem(lax.div(slot, at.cores), at.planes) + at.planes - at.plane, at.planes)
    sideways = lax.rem(in_plane + at.side - at.own, at.side)
    first = ((planes_on * at.side + sideways) * capacity).astype(F32)
    room_ids = lax.broadcasted_iota(jnp.int32, (tok_rows, room), 1)
    columns = []
    for k in range(top_count):
        columns += in_parts(column_of(probs_ref[k : k + 1, :]))
    for k, hit in enumerate(hits):
        place = jnp.sum(hit * (before + first), axis=1, keepdims=True).astype(jnp.int32)
        hots_ref[k] = (room_ids == place).astype(F32).astype(BF16)
        high = lax.div(place, capacity)
        columns += [high.astype(F32), (place - high * capacity).astype(F32)]
    tok[0, :, pl.ds(2 * width, LANES)] = in_lanes(columns)
    tok[0, :, pl.ds(0, width)] = tokens_ref[...]
    tok[0, :, pl.ds(width, width)] = grads_ref[...]

    half_rows = tok_rows // 2
    tok_sems = (tok_send, tok_recv)

    def block(d, h):
        return tok.at[d, pl.ds(h * half_rows, half_rows)]

    def to_plane(kind, h):
        up = at.member(0, 1)
        down = at.member(0, at.planes - 1)
        if kind == 2:
            source, device = (block(1, 0), up) if h == 0 else (block(3, 1), down)
            return send(source, block(2, h), tok_sems, (2, h), device)
        target = block(1, h) if kind == 0 else block(3, h)
        return send(block(0, h), target, tok_sems, (kind, h), up if kind == 0 else down)

    to_plane(0, 0).start()
    to_plane(1, 1).start()

    def row_copy(d, r):
        rows = pl.ds(pl.multiple_of(d * plane_room + r * capacity, capacity), capacity)
        n = d * at.side + r
        return send(
            send_ref.at[rows], recv.at[rows], (row_send, row_recv), n, at.member(r, 0)
        )

    def dispatch(d):
        lanes = tok[d, :, pl.ds(2 * width, LANES)]
        slots = lax.broadcasted_iota(jnp.int32, (tok_rows, plane_room), 1) + d * plane_room
        lane = lax.broadcasted_iota(jnp.int32, lanes.shape, 1)
        number = lanes.astype(F32)
        both = jnp.zeros((plane_room, tok_rows), F32)
        parts = jnp.zeros((plane_room, LANES), F32)
        for k in range(top_count):
            start = 3 * top_count + 2 * k
            place = number[:, start : start + 1] * capacity + number[:, start + 1 : start + 2]
            hot = (slots == place.astype(jnp.int32)).astype(F32).T
            both = both + hot
            own = jnp.where(lane >= 3 * k, jnp.where(lane < 3 * k + 3, number, 0.0), 0.0)
            parts = parts + dot(hot.astype(BF16), own.astype(BF16))
        rows = pl.ds(d * plane_room, plane_room)
        both = both.astype(BF16)
        step = min(512, width)
        for c in range(2 * width // step):
            columns = pl.ds(c * step, step)
            send_ref[rows, columns] = dot(both, tok[d, :, columns]).astype(BF16)
        send_ref[rows, pl.ds(2 * width, LANES)] = parts.astype(BF16)

        def start_row(r, carry):
            row_copy(d, r).start()
            return carry

        lax.fori_loop(1, at.side, start_row, 0)
        own_rows = pl.ds(d * plane_room, capacity)
        recv[own_rows] = send_ref[own_rows]

    dispatch(0)

    flag = swapped_here(pairs_ref, at.me, half_axis)
    gather = (gather_send, gather_recv)

    def shard(layer, step, c):
        start = at.shard(layer, step) * depth + c * part
        return full_ref.at[pl.ds(pl.multiple_of(start, part), part)]

    def spread(kind, layer, step, c, device):
        shared = shard(layer, step, c)
        return send(shared, shared, gather, (kind, c), device)

    spreading = []

    def begin_spread(*what):
        copy = spread(*what)
        copy.start()
        spreading.append(copy)

    ACROSS, UP_OWN, DOWN_OWN, UP_OTHER, DOWN_OTHER, UP_ON, DOWN_ON = range(7)

    def open_gather(c):
        for copy in swaps[c]:
            copy.wait_recv()
        rows = pl.ds(c * part, part)
        mine = shard(0, 0, c)
        new_in = choose(flag, swap_in[rows], w_in_ref[rows]).astype(BF16)
        new_down = choose(flag, swap_down[rows], w_down_ref[rows]).astype(BF16)
        mine[:, pl.ds(0, wide)] = new_in
        mine[:, pl.ds(wide, half_width)] = new_down
        weight_ref[rows, pl.ds(0, wide)] = new_in
        weight_ref[rows, pl.ds(wide, half_width)] = new_down
        begin_spread(ACROSS, 0, 0, c, at.across)
        begin_spread(UP_OWN, 0, 0, c, at.up)
        begin_spread(DOWN_OWN, 0, 0, c, at.down)

    def pass_own(c):
        spread(UP_OWN, 0, -1, c, at.up).wait_recv()
        begin_spread(UP_ON, 0, -1, c, at.up)

    def spread_other(c):
        spread(ACROSS, 1, 0, c, at.across).wait_recv()
        begin_spread(UP_OTHER, 1, 0, c, at.up)
        begin_spread(DOWN_OTHER, 1, 0, c, at.down)

    def pass_other(c):
        spread(DOWN_OTHER, 1, 1, c, at.down).wait_recv()
        begin_spread(DOWN_ON, 1, 1, c, at.down)

    chunks = range(GATHER_CHUNKS)
    middle = GATHER_CHUNKS // 2
    for c in chunks:
        open_gather(c)
    to_plane(0, 1).start()
    to_plane(1, 0).start()
    for c in chunks[:middle]:
        pass_own(c)
    to_plane(0, 0).wait_recv()
    to_plane(2, 0).start()
    to_plane(1, 1).wait_recv()
    to_plane(2, 1).start()
    for c in chunks[:middle]:
        spread_other(c)
    for c in chunks[middle:]:
        pass_own(c)
    for c in chunks[middle:]:
        spread_other(c)
    to_plane(0, 1).wait_recv()
    dispatch(1)
    for c in chunks[:middle]:
        pass_other(c)
    to_plane(1, 0).wait_recv()
    dispatch(3)
    for c in chunks[middle:]:
        pass_other(c)
    to_plane(2, 0).wait_recv()
    to_plane(2, 1).wait_recv()
    dispatch(2)

    moments = []
    for n, (own, other) in enumerate(
        ((m_in_ref, pm_in), (m_down_ref, pm_down), (v_in_ref, pv_in), (v_down_ref, pv_down))
    ):
        moments.append(send(own, other, (moment_send, moment_recv), n, partner))
        moments[-1].start()

    for c in chunks:
        spread(DOWN_OWN, 0, 1, c, at.down).wait_recv()
        spread(UP_OTHER, 1, -1, c, at.up).wait_recv()
        spread(UP_ON, 0, -2, c, at.up).wait_recv()
        spread(DOWN_ON, 1, 2, c, at.down).wait_recv()

    def wait_plane(d, carry):
        def wait_row(r, carry):
            row_copy(d, r).wait_recv()
            return carry

        return lax.fori_loop(1, at.side, wait_row, carry)

    lax.fori_loop(0, at.planes, wait_plane, 0)

    lanes = recv[:, 2 * width :]
    rows_p = from_parts(lanes)
    for k in range(1, top_count):
        rows_p = rows_p + from_parts(lanes, 3 * k)
    step = min(512, width)
    for c in range(width // step):
        columns = pl.ds(c * step, step)
        rows_g = recv[:, pl.ds(width + c * step, step)].astype(F32)
        scaled[:, columns] = (rows_p * rows_g).astype(BF16)
    span = min(256, half_width)

    def through(n, carry):
        gate_at = pl.multiple_of(n * span, span)
        up_at = pl.multiple_of(half_width + n * span, span)
        down_at = pl.multiple_of(wide + n * span, span)
        gate_part = dot(recv[:, :width], full_ref[:, pl.ds(gate_at, span)])
        up_part = dot(recv[:, :width], full_ref[:, pl.ds(up_at, span)])
        hidden_grad = dot(scaled[...], full_ref[:, pl.ds(down_at, span)])
        sigmoid = jax.nn.sigmoid(gate_part)
        activated = gate_part * sigmoid
        slope_term = sigmoid * (1.0 + gate_part * (1.0 - sigmoid))
        hidden[:, pl.ds(gate_at, span)] = (activated * up_part).astype(BF16)
        pre[:, pl.ds(gate_at, span)] = (hidden_grad * up_part * slope_term).astype(BF16)
        pre[:, pl.ds(up_at, span)] = (hidden_grad * activated).astype(BF16)
        return carry

    lax.fori_loop(0, half_width // span, through, 0)

    def weight_grads(i, carry):
        start = pl.multiple_of(at.shard(i % 2, 2 + i // 2) * depth, depth)
        columns = pl.ds(start, depth)
        grad[i, :, pl.ds(0, wide)] = dot(recv[:, columns], pre[...], (0, 0)).astype(BF16)
        grad[i, :, pl.ds(wide, half_width)] = dot(
            scaled[:, columns], hidden[...], (0, 0)
        ).astype(BF16)
        return carry

    ring = (ring_send, ring_recv)
    summing = []
    part = depth // SUM_CHUNKS

    def begin(source, target, kind, c, device):
        copy = send(source, target.at[c], ring, (kind, c), device)
        copy.start()
        summing.append(copy)

    def arrived(target, kind, c):
        send(target.at[c], target.at[c], ring, (kind, c), at.up).wait_recv()
        return target[c].astype(F32)

    def rows_of(c):
        return pl.ds(c * part, part)

    A2, B2, A3, B3, A0, B0, A1, B1 = range(8)
    ON_UP, ON_DOWN, A_LOW, A_HIGH, B_LOW, B_HIGH, Z = range(7)
    lax.fori_loop(0, 2, weight_grads, 0)
    for c in range(SUM_CHUNKS):
        begin(grad.at[A2, rows_of(c)], on_up, ON_UP, c, at.up)
        begin(grad.at[B2, rows_of(c)], on_down, ON_DOWN, c, at.down)
    lax.fori_loop(2, 8, weight_grads, 0)
    early = SUM_CHUNKS // 2
    for c in range(early):
        begin(grad.at[B1, rows_of(c)], b_low, B_LOW, c, at.up)
        begin(grad.at[A3, rows_of(c)], a_high, A_HIGH, c, at.down)

    span_out = min(256, width)

    def row_grads(n, total):
        start = pl.multiple_of(n * span_out, span_out)
        rows = pl.ds(start, span_out)
        ret[:, rows] = dot(pre[...], full_ref[rows, pl.ds(0, wide)], (1, 1)).astype(BF16)
        out = dot(hidden[...], full_ref[rows, pl.ds(wide, half_width)], (1, 1)).astype(BF16)
        rows_g = recv[:, pl.ds(pl.multiple_of(width + start, span_out), span_out)].astype(F32)
        return total + jnp.sum(out.astype(F32) * rows_g, axis=1, keepdims=True)

    row_total = lax.fori_loop(0, width // span_out, row_grads, jnp.zeros((room, 1), F32))
    ret[:, width:] = in_lanes(in_parts(row_total))

    def rows_to(i):
        k = at.offset(i)
        rows = pl.ds(pl.multiple_of(k * capacity, capacity), capacity)
        device = at.member(at.side - k % at.side, at.planes - k // at.side)
        return send(ret.at[rows], back.at[rows], (back_send, back_recv), k, device)

    def start_rows(i, carry):
        rows_to(i).start()
        return carry

    def wait_rows(i, carry):
        rows_to(i).wait()
        return carry

    lax.fori_loop(1, experts, start_rows, 0)
    back[0:capacity] = ret[0:capacity]

    def pass_on(c):
        low = grad[A1, rows_of(c)].astype(F32) + arrived(on_up, ON_UP, c)
        grad[A1, rows_of(c)] = low.astype(BF16)
        begin(grad.at[A1, rows_of(c)], a_low, A_LOW, c, at.up)
        high = grad[B3, rows_of(c)].astype(F32) + arrived(on_down, ON_DOWN, c)
        grad[B3, rows_of(c)] = high.astype(BF16)
        begin(grad.at[B3, rows_of(c)], b_high, B_HIGH, c, at.down)

    for c in range(SUM_CHUNKS):
        pass_on(c)
        if c + early < SUM_CHUNKS:
            begin(grad.at[B1, rows_of(c + early)], b_low, B_LOW, c + early, at.up)
            begin(grad.at[A3, rows_of(c + early)], a_high, A_HIGH, c + early, at.down)

    def hand_over(c):
        mine = grad[B0, rows_of(c)].astype(F32)
        mine = mine + arrived(b_low, B_LOW, c) + arrived(b_high, B_HIGH, c)
        grad[B0, rows_of(c)] = mine.astype(BF16)
        begin(grad.at[B0, rows_of(c)], z_in, Z, c, at.across)

    def add_up(c):
        mine = grad[A0, rows_of(c)].astype(F32)
        mine = mine + arrived(a_low, A_LOW, c) + arrived(a_high, A_HIGH, c)
        total_ref[rows_of(c)] = mine + arrived(z_in, Z, c)

    for c in range(SUM_CHUNKS):
        hand_over(c)
        if c > 0:
            add_up(c - 1)
    add_up(SUM_CHUNKS - 1)
    lax.fori_loop(1, experts, wait_rows, 0)
    for copy in moments:
        copy.wait()

    def wait_sent(d, carry):
        def wait_row(r, carry):
            row_copy(d, r).wait_send()
            return carry

        return lax.fori_loop(1, at.side, wait_row, carry)

    lax.fori_loop(0, at.planes, wait_sent, 0)
    for kind in range(3):
        for h in range(2):
            to_plane(kind, h).wait_send()
    for pair in swaps:
        for copy in pair:
            copy.wait_send()
    for copy in spreading + summing:
        copy.wait_send()


def update_kernel(
    pairs_ref, total_ref, weight_ref, back, back_lanes, hots_ref,
    m_in_ref, m_down_ref, v_in_ref, v_down_ref, pm_in, pm_down, pv_in, pv_down,
    token_ref, prob_ref, nw_in, nw_down, nm_in, nm_down, nv_in, nv_down,
):
    at = Place()
    flag = swapped_here(pairs_ref, at.me, at.experts // 2)
    wide, half_width = m_in_ref.shape[1], m_down_ref.shape[1]
    for start, size, refs in (
        (0, wide, (pm_in, m_in_ref, pv_in, v_in_ref, nw_in, nm_in, nv_in)),
        (wide, half_width, (pm_down, m_down_ref, pv_down, v_down_ref, nw_down, nm_down, nv_down)),
    ):
        columns = pl.ds(start, size)
        value = total_ref[:, columns]
        first = choose(flag, refs[0][...], refs[1][...])
        second = choose(flag, refs[2][...], refs[3][...])
        weight = weight_ref[:, columns].astype(F32)
        first_new = beta_one * first + (1.0 - beta_one) * value
        second_new = beta_two * second + (1.0 - beta_two) * value * value
        step_size = first_new / bias_one / (jnp.sqrt(second_new / bias_two) + adam_eps)
        refs[4][...] = (weight - learn_rate * step_size).astype(BF16)
        refs[5][...] = first_new.astype(BF16)
        refs[6][...] = second_new.astype(BF16)
    hots = [hots_ref[k] for k in range(hots_ref.shape[0])]
    both = hots[0]
    for hot in hots[1:]:
        both = both + hot
    token_ref[...] = dot(both, back[...]).astype(BF16)

    @pl.when(pl.program_id(0) == 0)
    def _():
        for k, hot in enumerate(hots):
            prob_ref[:, k : k + 1] = from_parts(dot(hot, back_lanes[...]))


def body(
    tokens,
    out_grad,
    expert_ids,
    gate_probs,
    held_expert,
    swap_pairs,
    w_in,
    w_down,
    m_in,
    m_down,
    v_in,
    v_down,
):
    experts = lax.axis_size(EXPERT)
    planes, side = lax.axis_size("ez"), experts // lax.axis_size("ez")
    dp = lax.axis_size(DP)
    tok_rows, width = tokens.shape
    top_count = expert_ids.shape[1]
    capacity = max(2, 2 * tok_rows * top_count // experts)
    room = experts * capacity
    _, depth, wide = w_in.shape
    half_width = w_down.shape[2]
    joint = wide + half_width
    row_width = 2 * width + LANES
    vmem = pl.BlockSpec(memory_space=pltpu.VMEM)
    smem = pl.BlockSpec(memory_space=pltpu.SMEM)
    anywhere = pl.BlockSpec(memory_space=pl.ANY)
    dma = pltpu.SemaphoreType.DMA
    shape = jax.ShapeDtypeStruct
    chunked = pltpu.VMEM((SUM_CHUNKS, depth // SUM_CHUNKS, joint), BF16)
    state_in, state_down = shape((depth, wide), BF16), shape((depth, half_width), BF16)
    moments = (m_in[0], m_down[0], v_in[0], v_down[0])
    total, weight, back, hots, *moved = pl.pallas_call(
        layer_kernel,
        name="layer",
        out_shape=(
            shape((depth, joint), F32),
            shape((depth, joint), BF16),
            shape((room, width + LANES), BF16),
            shape((top_count, tok_rows, room), BF16),
        )
        + (state_in, state_down) * 2,
        in_specs=[vmem, vmem, smem] + [vmem] * 5 + [anywhere] * 4,
        out_specs=(vmem,) * 4 + (anywhere,) * 4,
        scratch_shapes=[
            pltpu.VMEM((planes, tok_rows, row_width), BF16),
            pltpu.VMEM((room, row_width), BF16),
            pltpu.VMEM((room, row_width), BF16),
            pltpu.VMEM((dp * depth, joint), BF16),
            pltpu.VMEM((depth, wide), BF16),
            pltpu.VMEM((depth, half_width), BF16),
            pltpu.VMEM((room, width), BF16),
            pltpu.VMEM((room, wide), BF16),
            pltpu.VMEM((room, half_width), BF16),
            pltpu.VMEM((dp, depth, joint), BF16),
            pltpu.VMEM((room, width + LANES), BF16),
        ]
        + [chunked] * 7
        + [dma((3, 2))] * 2
        + [dma((experts,))] * 4
        + [dma((2, GATHER_CHUNKS))] * 2
        + [dma((4,))] * 2
        + [dma((7, GATHER_CHUNKS))] * 2
        + [dma((7, SUM_CHUNKS))] * 2,
        compiler_params=pltpu.CompilerParams(
            collective_id=0, has_side_effects=True, vmem_limit_bytes=VMEM_BYTES
        ),
    )(
        expert_ids.T,
        held_expert.reshape(1, experts),
        swap_pairs,
        gate_probs.T,
        tokens,
        out_grad,
        w_in[0],
        w_down[0],
        *moments,
    )
    steps = ADAM_STEPS

    def rows(columns):
        return pl.BlockSpec((depth // steps, columns), lambda i: (i, 0))

    states = [rows(wide), rows(half_width)]
    result = pl.pallas_call(
        update_kernel,
        name="update",
        grid=(steps,),
        out_shape=(shape((tok_rows, width), BF16), shape((tok_rows, top_count), F32))
        + (state_in, state_down) * 3,
        in_specs=[
            smem,
            rows(joint),
            rows(joint),
            pl.BlockSpec((room, width // steps), lambda i: (0, i)),
            pl.BlockSpec((room, LANES), lambda i: (0, width // LANES)),
            pl.BlockSpec((top_count, tok_rows, room), lambda i: (0, 0, 0)),
        ]
        + states * 4,
        out_specs=[
            pl.BlockSpec((tok_rows, width // steps), lambda i: (0, i)),
            pl.BlockSpec((tok_rows, top_count), lambda i: (0, 0)),
        ]
        + states * 3,
    )(swap_pairs, total, weight, back, back, hots, *moments, *moved)
    return tuple(result[:2]) + tuple(r[None] for r in result[2:])


def solution(mesh):
    experts = mesh.shape["expert"]
    shape = (2, 4, experts // 8, 4, 2)
    split = Mesh(mesh.devices.reshape(shape), DP_EXPERT)
    rows = P(DP_EXPERT, None)
    state = P(EXPERT, DP, None)
    return jax.shard_map(
        body,
        mesh=split,
        in_specs=(rows,) * 4 + (P(), P()) + (state,) * 6,
        out_specs=(rows, rows) + (state,) * 6,
        check_vma=False,
    )
```

```python
import functools

import jax
import jax.numpy as jnp
from jax import lax
from jax.experimental import pallas as pl
from jax.experimental.pallas import tpu as pltpu
from jax.sharding import Mesh
from jax.sharding import PartitionSpec as P

DP = ("dp_0", "dp_1")
EXPERT = ("ex", "ez", "ec")
DP_EXPERT = DP + EXPERT
MESH = pl.DeviceIdType.MESH
BF16, F32 = jnp.bfloat16, jnp.float32

beta_one = 0.9
beta_two = 0.95
learn_rate = 0.01
adam_eps = 1e-08
bias_one = 1.0 - 0.9**10
bias_two = 1.0 - 0.95**10

LANES = 128
PART_UNITS = 256
HALVES = 2
ADAM_STEPS = 4
VMEM_BYTES = 60 * 1024 * 1024


def in_parts(column):
    high = column.astype(BF16).astype(F32)
    rest = column - high
    middle = rest.astype(BF16).astype(F32)
    return [high, middle, rest - middle]


def in_lanes(columns):
    lane = lax.broadcasted_iota(jnp.int32, (columns[0].shape[0], LANES), 1)
    result = jnp.zeros(lane.shape, F32)
    for n, column in enumerate(columns):
        result = jnp.where(lane == n, column, result)
    return result.astype(BF16)


def from_parts(parts, start=0):
    parts = parts.astype(F32)
    high, middle, low = (parts[:, start + n : start + n + 1] for n in range(3))
    return high + middle + low


def column_of(row, turn=0):
    n = row.shape[1]
    at, lane = (lax.broadcasted_iota(jnp.int32, (n, n), d) for d in (0, 1))
    return jnp.sum(jnp.where(lane == lax.rem(at + turn, n), row, 0.0), axis=1, keepdims=True)


def row_of(column):
    n = column.shape[0]
    at, lane = (lax.broadcasted_iota(jnp.int32, (n, n), d) for d in (0, 1))
    return jnp.sum(jnp.where(lane == at, column, 0.0), axis=0, keepdims=True)


def dot(a, b, contract=(1, 0)):
    dims = (((contract[0],), (contract[1],)), ((), ()))
    return lax.dot_general(a, b, dims, preferred_element_type=F32)


def swapped_here(pairs_ref, me, half_axis):
    mine = lax.rem(me, half_axis)
    flag = (mine == pairs_ref[0]).astype(jnp.int32)
    for j in range(1, pairs_ref.shape[0]):
        flag = jnp.maximum(flag, (mine == pairs_ref[j]).astype(jnp.int32))
    return flag


def choose(flag, moved, kept):
    return jnp.where(jnp.full(kept.shape, flag, jnp.int32) > 0, moved.astype(F32), kept.astype(F32))


def send(source, target, sems, at, device):
    return pltpu.make_async_remote_copy(
        src_ref=source,
        dst_ref=target,
        send_sem=sems[0].at[at],
        recv_sem=sems[1].at[at],
        device_id=device,
        device_id_type=MESH,
    )


class Place:
    def __init__(self):
        self.z, self.y = lax.axis_index("dp_0"), lax.axis_index("dp_1")
        self.layers, self.ring = lax.axis_size("dp_0"), lax.axis_size("dp_1")
        self.cores, self.planes = lax.axis_size("ec"), lax.axis_size("ez")
        self.side = lax.axis_size("ex") * self.cores
        self.experts = self.side * self.planes
        self.own = lax.axis_index("ex") * self.cores + lax.axis_index("ec")
        self.plane = lax.axis_index("ez")
        self.me = (
            lax.axis_index("ex") * self.planes + self.plane
        ) * self.cores + lax.axis_index("ec")
        self.across = {"dp_0": 1 - self.z}
        self.up = {"dp_1": lax.rem(self.y + 1, self.ring)}
        self.down = {"dp_1": lax.rem(self.y + self.ring - 1, self.ring)}

    def member(self, sideways, planes):
        q = (self.own + sideways) % self.side
        z = (self.plane + planes) % self.planes
        return {"ex": q // self.cores, "ez": z, "ec": q % self.cores}

    def partner(self):
        e = (self.me + self.experts // 2) % self.experts
        return {
            "ex": e // (self.planes * self.cores),
            "ez": (e // self.cores) % self.planes,
            "ec": e % self.cores,
        }

    def offset(self, i):
        return (i % 2) * ((i + 1) // 2) + (1 - i % 2) * (self.experts - i // 2)

    def shard(self, layer, step):
        z = (self.z + layer) % self.layers
        return z * self.ring + (self.y + step) % self.ring

    def greet(self):
        barrier = pltpu.get_barrier_semaphore()

        def hello(k, carry):
            device = self.member(k % self.side, k // self.side)
            pl.semaphore_signal(barrier, inc=1, device_id=device, device_id_type=MESH)
            return carry

        lax.fori_loop(1, self.experts, hello, 0)
        for device in (self.across, self.up, self.down):
            pl.semaphore_signal(barrier, inc=1, device_id=device, device_id_type=MESH)
        pl.semaphore_wait(barrier, self.experts - 1 + 3)


def layer_kernel(
    ids_ref, held_ref, pairs_ref, probs_ref, tokens_ref, grads_ref, w_in_ref, w_down_ref,
    m_in_ref, m_down_ref, v_in_ref, v_down_ref,
    total_ref, weight_ref, back, hots_ref, pm_in, pm_down, pv_in, pv_down,
    tok, send_ref, recv, full_ref, swap_in, swap_down, scaled, x_turned, s_turned, pre, hidden, grad,
    on_up, on_down, a_low, a_high, b_low, b_high, z_in,
    tok_send, tok_recv, row_send, row_recv, back_send, back_recv, swap_send, swap_recv,
    moment_send, moment_recv, gather_send, gather_recv, ring_send, ring_recv,
):
    at = Place()
    experts, half_axis = at.experts, at.experts // 2
    tok_rows, width = tokens_ref.shape
    room, row_width = recv.shape
    capacity = room // experts
    plane_room = room // at.planes
    depth, wide = w_in_ref.shape
    half_width = w_down_ref.shape[1]
    at.greet()

    half_rows = tok_rows // 2
    tok_sems = (tok_send, tok_recv)
    plane_up, plane_down = at.member(0, 1), at.member(0, at.planes - 1)
    pieces = (pl.ds(0, width), pl.ds(width, width), pl.ds(2 * width, LANES))

    def block(d, h, piece):
        return tok.at[d, pl.ds(h * half_rows, half_rows), pieces[piece]]

    def to_plane(kind, h, piece):
        if kind == 2:
            source, device = (block(1, 0, piece), plane_up) if h == 0 else (block(3, 1, piece), plane_down)
            target = block(2, h, piece)
        else:
            rows = pl.ds(h * half_rows, half_rows)
            source = (tokens_ref.at[rows], grads_ref.at[rows], block(0, h, piece))[piece]
            target, device = (block(1, h, piece), plane_up) if kind == 0 else (block(3, h, piece), plane_down)
        return send(source, target, tok_sems, (kind, h, piece), device)

    for piece in range(2):
        to_plane(0, 0, piece).start()
        to_plane(1, 1, piece).start()

    span = min(PART_UNITS, half_width)
    parts = half_width // span
    partner = at.partner()
    sems = (swap_send, swap_recv)
    swaps = []
    for c in range(parts):
        gate, up = pl.ds(c * span, span), pl.ds(half_width + c * span, span)
        swaps.append(
            (
                send(w_in_ref.at[:, gate], swap_in.at[:, gate], sems, (0, c), partner),
                send(w_in_ref.at[:, up], swap_in.at[:, up], sems, (1, c), partner),
                send(w_down_ref.at[:, gate], swap_down.at[:, gate], sems, (2, c), partner),
            )
        )
        for copy in swaps[-1]:
            copy.start()

    slot = lax.broadcasted_iota(jnp.int32, (1, experts), 1)
    flag = (lax.rem(slot, half_axis) == pairs_ref[0]).astype(jnp.int32)
    for j in range(1, pairs_ref.shape[0]):
        flag = jnp.maximum(flag, (lax.rem(slot, half_axis) == pairs_ref[j]).astype(jnp.int32))
    before_swap = held_ref[...].astype(F32)
    held = jnp.where(flag > 0, row_of(column_of(before_swap, half_axis)), before_swap)
    top_count = ids_ref.shape[0]
    hits = [
        (column_of(ids_ref[k : k + 1, :].astype(F32)) == held).astype(F32)
        for k in range(top_count)
    ]
    named = hits[0]
    for hit in hits[1:]:
        named = named + hit
    row, column = (lax.broadcasted_iota(jnp.int32, (tok_rows, tok_rows), d) for d in (0, 1))
    before = dot((column < row).astype(F32).astype(BF16), named.astype(BF16))
    in_plane = lax.div(slot, at.planes * at.cores) * at.cores + lax.rem(slot, at.cores)
    planes_on = lax.rem(lax.rem(lax.div(slot, at.cores), at.planes) + at.planes - at.plane, at.planes)
    sideways = lax.rem(in_plane + at.side - at.own, at.side)
    first = ((planes_on * at.side + sideways) * capacity).astype(F32)
    room_ids = lax.broadcasted_iota(jnp.int32, (tok_rows, room), 1)
    columns = []
    for k in range(top_count):
        columns += in_parts(column_of(probs_ref[k : k + 1, :]))
    for k, hit in enumerate(hits):
        place = jnp.sum(hit * (before + first), axis=1, keepdims=True).astype(jnp.int32)
        hots_ref[k] = (room_ids == place).astype(F32).astype(BF16)
        high = lax.div(place, capacity)
        columns += [high.astype(F32), (place - high * capacity).astype(F32)]
    tok[0, :, pl.ds(2 * width, LANES)] = in_lanes(columns)
    to_plane(0, 0, 2).start()
    to_plane(1, 1, 2).start()

    def row_copy(d, r):
        rows = pl.ds(pl.multiple_of(d * plane_room + r * capacity, capacity), capacity)
        n = d * at.side + r
        return send(
            send_ref.at[rows], recv.at[rows], (row_send, row_recv), n, at.member(r, 0)
        )

    def dispatch(d):
        lanes = tok[d, :, pl.ds(2 * width, LANES)]
        slots = lax.broadcasted_iota(jnp.int32, (tok_rows, plane_room), 1) + d * plane_room
        lane = lax.broadcasted_iota(jnp.int32, lanes.shape, 1)
        number = lanes.astype(F32)
        both = jnp.zeros((plane_room, tok_rows), F32)
        values = jnp.zeros((plane_room, LANES), F32)
        for k in range(top_count):
            start = 3 * top_count + 2 * k
            place = number[:, start : start + 1] * capacity + number[:, start + 1 : start + 2]
            hot = (slots == place.astype(jnp.int32)).astype(F32).T
            both = both + hot
            own = jnp.where(lane >= 3 * k, jnp.where(lane < 3 * k + 3, number, 0.0), 0.0)
            values = values + dot(hot.astype(BF16), own.astype(BF16))
        rows = pl.ds(d * plane_room, plane_room)
        both = both.astype(BF16)
        step = min(512, width)
        for c in range(2 * width // step):
            columns = pl.ds(c * step, step)
            if d > 0:
                source = tok[d, :, columns]
            elif c * step < width:
                source = tokens_ref[:, columns]
            else:
                source = grads_ref[:, pl.ds(c * step - width, step)]
            send_ref[rows, columns] = dot(both, source).astype(BF16)
        send_ref[rows, pl.ds(2 * width, LANES)] = values.astype(BF16)

        def start_row(r, carry):
            row_copy(d, r).start()
            return carry

        lax.fori_loop(1, at.side, start_row, 0)
        own_rows = pl.ds(d * plane_room, capacity)
        recv[own_rows] = send_ref[own_rows]

    def take_rows(d):
        def wait_row(r, carry):
            row_copy(d, r).wait_recv()
            return carry

        lax.fori_loop(1, at.side, wait_row, 0)
        rows = pl.ds(d * plane_room, plane_room)
        lanes = recv[rows, pl.ds(2 * width, LANES)]
        rows_p = from_parts(lanes)
        for k in range(1, top_count):
            rows_p = rows_p + from_parts(lanes, 3 * k)
        step = min(512, width)
        for c in range(width // step):
            columns = pl.ds(c * step, step)
            rows_g = recv[rows, pl.ds(width + c * step, step)].astype(F32)
            rows_s = (rows_p * rows_g).astype(BF16)
            scaled[rows, columns] = rows_s
            s_turned[columns, rows] = rows_s.T
            x_turned[columns, rows] = recv[rows, columns].T

    dispatch(0)

    flag = swapped_here(pairs_ref, at.me, half_axis)
    gather = (gather_send, gather_recv)

    def shard(layer, step, c):
        start = at.shard(layer, step) * depth
        return full_ref.at[c, pl.ds(pl.multiple_of(start, depth), depth)]

    def spread(kind, layer, step, c, device):
        shared = shard(layer, step, c)
        return send(shared, shared, gather, (kind, c), device)

    spreading = []

    def begin_spread(*what):
        copy = spread(*what)
        copy.start()
        spreading.append(copy)

    ACROSS, UP_OWN, DOWN_OWN, UP_OTHER, DOWN_OTHER, UP_ON, DOWN_ON = range(7)

    def open_gather(c):
        for copy in swaps[c]:
            copy.wait_recv()
        mine = shard(0, 0, c)
        for n, (here, there, start) in enumerate(
            ((w_in_ref, swap_in, 0), (w_in_ref, swap_in, half_width), (w_down_ref, swap_down, 0))
        ):
            columns = pl.ds(start + c * span, span)
            new = choose(flag, there[:, columns], here[:, columns]).astype(BF16)
            mine[:, pl.ds(n * span, span)] = new
            weight_ref[:, pl.ds(n * half_width + c * span, span)] = new
        begin_spread(UP_OWN, 0, 0, c, at.up)
        begin_spread(DOWN_OWN, 0, 0, c, at.down)

    def cross(c):
        begin_spread(ACROSS, 0, 0, c, at.across)

    def pass_own(c):
        spread(UP_OWN, 0, -1, c, at.up).wait_recv()
        begin_spread(UP_ON, 0, -1, c, at.up)

    def spread_other(c):
        spread(ACROSS, 1, 0, c, at.across).wait_recv()
        begin_spread(UP_OTHER, 1, 0, c, at.up)
        begin_spread(DOWN_OTHER, 1, 0, c, at.down)

    def pass_other(c):
        spread(DOWN_OTHER, 1, 1, c, at.down).wait_recv()
        begin_spread(DOWN_ON, 1, 1, c, at.down)

    every = range(parts)

    def more_blocks():
        for piece in range(3):
            to_plane(0, 1, piece).start()
            to_plane(1, 0, piece).start()

    def pass_blocks():
        for kind, h in ((0, 0), (1, 1)):
            for piece in range(3):
                to_plane(kind, h, piece).wait_recv()
            for piece in range(3):
                to_plane(2, h, piece).start()

    def spread_block(d):
        for kind, h in {1: ((0, 1),), 3: ((1, 0),), 2: ((2, 0), (2, 1))}[d]:
            for piece in range(3):
                to_plane(kind, h, piece).wait_recv()
        dispatch(d)

    pairs_of = ((m_in_ref, pm_in), (m_down_ref, pm_down), (v_in_ref, pv_in), (v_down_ref, pv_down))
    moments = [
        send(own, other, (moment_send, moment_recv), n, partner)
        for n, (own, other) in enumerate(pairs_of)
    ]
    for c in every:
        open_gather(c)
        cross(c)
    more_blocks()
    for c in every[:-1]:
        pass_own(c)
    pass_blocks()
    for c in every[:-1]:
        spread_other(c)
    pass_own(parts - 1)
    spread_other(parts - 1)
    spread_block(1)
    pass_other(0)
    spread_block(3)
    for c in every[1:]:
        pass_other(c)
    spread_block(2)
    for copy in moments[:2]:
        copy.start()

    def gathered(c):
        spread(DOWN_OWN, 0, 1, c, at.down).wait_recv()
        spread(UP_OTHER, 1, -1, c, at.up).wait_recv()
        spread(UP_ON, 0, -2, c, at.up).wait_recv()
        spread(DOWN_ON, 1, 2, c, at.down).wait_recv()

    for d in (0, 1, 3):
        take_rows(d)
    gathered(0)
    take_rows(2)

    ring = (ring_send, ring_recv)
    summing = []
    part = depth // HALVES

    def begin(source, target, kind, c, device):
        copy = send(source, target.at[c], ring, (kind, c), device)
        copy.start()
        summing.append(copy)

    def arrived(target, kind, c):
        send(target.at[c], target.at[c], ring, (kind, c), at.up).wait_recv()
        return target[c].astype(F32)

    def piece_of(i, c):
        return grad.at[c // HALVES, i, pl.ds((c % HALVES) * part, part)]

    A2, B2, A3, B3, A0, B0, A1, B1 = range(8)
    ON_UP, ON_DOWN, A_LOW, A_HIGH, B_LOW, B_HIGH, Z = range(7)

    def through(n):
        gate_part = dot(recv[:, :width], full_ref[n, :, pl.ds(0, span)])
        up_part = dot(recv[:, :width], full_ref[n, :, pl.ds(span, span)])
        hidden_grad = dot(scaled[...], full_ref[n, :, pl.ds(2 * span, span)])
        sigmoid = jax.nn.sigmoid(gate_part)
        activated = gate_part * sigmoid
        slope_term = sigmoid * (1.0 + gate_part * (1.0 - sigmoid))
        hidden[n] = (activated * up_part).astype(BF16)
        pre[n, :, pl.ds(0, span)] = (hidden_grad * up_part * slope_term).astype(BF16)
        pre[n, :, pl.ds(span, span)] = (hidden_grad * activated).astype(BF16)

    def sum_up(n):
        def weight_grads(i, carry):
            start = pl.multiple_of(at.shard(i % 2, 2 + i // 2) * depth, depth)
            rows = pl.ds(start, depth)
            grad[n, i, :, pl.ds(0, 2 * span)] = dot(x_turned[rows], pre[n]).astype(BF16)
            grad[n, i, :, pl.ds(2 * span, span)] = dot(s_turned[rows], hidden[n]).astype(BF16)
            return carry

        pieces_here = range(n * HALVES, (n + 1) * HALVES)
        lax.fori_loop(0, 2, weight_grads, 0)
        for c in pieces_here:
            begin(piece_of(A2, c), on_up, ON_UP, c, at.up)
            begin(piece_of(B2, c), on_down, ON_DOWN, c, at.down)
        lax.fori_loop(2, 8, weight_grads, 0)
        for c in pieces_here:
            begin(piece_of(B1, c), b_low, B_LOW, c, at.up)
            begin(piece_of(A3, c), a_high, A_HIGH, c, at.down)

    for n in every:
        if n > 0:
            gathered(n)
        through(n)
        if n == 0:
            sum_up(n)

    def wait_sent(d, carry):
        def wait_row(r, carry):
            row_copy(d, r).wait_send()
            return carry

        return lax.fori_loop(1, at.side, wait_row, carry)

    lax.fori_loop(0, at.planes, wait_sent, 0)

    span_out = min(256, width)

    ret = send_ref

    def row_grads(i, total):
        start = pl.multiple_of(i * span_out, span_out)
        rows = pl.ds(start, span_out)
        row_grad = jnp.zeros((room, span_out), F32)
        out = jnp.zeros((room, span_out), F32)
        for n in every:
            row_grad = row_grad + dot(pre[n], full_ref[n, rows, pl.ds(0, 2 * span)], (1, 1))
            out = out + dot(hidden[n], full_ref[n, rows, pl.ds(2 * span, span)], (1, 1))
        ret[:, rows] = row_grad.astype(BF16)
        rows_g = recv[:, pl.ds(pl.multiple_of(width + start, span_out), span_out)].astype(F32)
        return total + jnp.sum(out.astype(BF16).astype(F32) * rows_g, axis=1, keepdims=True)

    row_total = lax.fori_loop(0, width // span_out, row_grads, jnp.zeros((room, 1), F32))
    ret[:, pl.ds(width, LANES)] = in_lanes(in_parts(row_total))

    def rows_to(i):
        k = at.offset(i)
        rows = pl.ds(pl.multiple_of(k * capacity, capacity), capacity)
        device = at.member(at.side - k % at.side, at.planes - k // at.side)
        source = ret.at[rows, pl.ds(0, width + LANES)]
        return send(source, back.at[rows], (back_send, back_recv), k, device)

    def start_rows(i, carry):
        rows_to(i).start()
        return carry

    def wait_rows(i, carry):
        rows_to(i).wait()
        return carry

    lax.fori_loop(1, experts, start_rows, 0)
    for copy in moments[2:]:
        copy.start()
    back[0:capacity] = ret[0:capacity, pl.ds(0, width + LANES)]

    for n in every[1:]:
        sum_up(n)

    def pass_on(c):
        low, high = piece_of(A1, c), piece_of(B3, c)
        low[...] = (low[...].astype(F32) + arrived(on_up, ON_UP, c)).astype(BF16)
        begin(low, a_low, A_LOW, c, at.up)
        high[...] = (high[...].astype(F32) + arrived(on_down, ON_DOWN, c)).astype(BF16)
        begin(high, b_high, B_HIGH, c, at.down)

    def hand_over(c):
        other = piece_of(B0, c)
        mine = other[...].astype(F32) + arrived(b_low, B_LOW, c) + arrived(b_high, B_HIGH, c)
        other[...] = mine.astype(BF16)
        begin(other, z_in, Z, c, at.across)

    def add_up(c):
        mine = piece_of(A0, c)[...].astype(F32)
        mine = mine + arrived(a_low, A_LOW, c) + arrived(a_high, A_HIGH, c)
        mine = mine + arrived(z_in, Z, c)
        rows = pl.ds((c % HALVES) * part, part)
        for n in range(3):
            columns = pl.ds(n * half_width + c // HALVES * span, span)
            total_ref[rows, columns] = mine[:, n * span : (n + 1) * span]

    count = parts * HALVES
    for c in range(count):
        pass_on(c)
    for c in range(count):
        hand_over(c)
        if c > 0:
            add_up(c - 1)
    add_up(count - 1)
    lax.fori_loop(1, experts, wait_rows, 0)
    for copy in moments:
        copy.wait()

    for kind in range(3):
        for h in range(2):
            for piece in range(3):
                to_plane(kind, h, piece).wait_send()
    for pair in swaps:
        for copy in pair:
            copy.wait_send()
    for copy in spreading + summing:
        copy.wait_send()


def update_kernel(
    pairs_ref, total_ref, weight_ref, back, back_lanes, hots_ref,
    m_in_ref, m_down_ref, v_in_ref, v_down_ref, pm_in, pm_down, pv_in, pv_down,
    token_ref, prob_ref, nw_in, nw_down, nm_in, nm_down, nv_in, nv_down,
):
    at = Place()
    flag = swapped_here(pairs_ref, at.me, at.experts // 2)
    wide, half_width = m_in_ref.shape[1], m_down_ref.shape[1]
    for start, size, refs in (
        (0, wide, (pm_in, m_in_ref, pv_in, v_in_ref, nw_in, nm_in, nv_in)),
        (wide, half_width, (pm_down, m_down_ref, pv_down, v_down_ref, nw_down, nm_down, nv_down)),
    ):
        columns = pl.ds(start, size)
        value = total_ref[:, columns]
        first = choose(flag, refs[0][...], refs[1][...])
        second = choose(flag, refs[2][...], refs[3][...])
        weight = weight_ref[:, columns].astype(F32)
        first_new = beta_one * first + (1.0 - beta_one) * value
        second_new = beta_two * second + (1.0 - beta_two) * value * value
        root = jnp.sqrt(second_new * (1.0 / bias_two)) + adam_eps
        step_size = first_new * (1.0 / bias_one) / root
        refs[4][...] = (weight - learn_rate * step_size).astype(BF16)
        refs[5][...] = first_new.astype(BF16)
        refs[6][...] = second_new.astype(BF16)
    hots = [hots_ref[k] for k in range(hots_ref.shape[0])]
    both = hots[0]
    for hot in hots[1:]:
        both = both + hot
    token_ref[...] = dot(both, back[...]).astype(BF16)

    @pl.when(pl.program_id(0) == 0)
    def _():
        for k, hot in enumerate(hots):
            prob_ref[k : k + 1, :] = row_of(from_parts(dot(hot, back_lanes[...])))


def body(
    tokens,
    out_grad,
    expert_ids,
    gate_probs,
    held_expert,
    swap_pairs,
    w_in,
    w_down,
    m_in,
    m_down,
    v_in,
    v_down,
):
    experts = lax.axis_size(EXPERT)
    planes, side = lax.axis_size("ez"), experts // lax.axis_size("ez")
    dp = lax.axis_size(DP)
    tok_rows, width = tokens.shape
    top_count = expert_ids.shape[1]
    capacity = max(2, 2 * tok_rows * top_count // experts)
    room = experts * capacity
    _, depth, wide = w_in.shape
    half_width = w_down.shape[2]
    joint = wide + half_width
    row_width = 2 * width + LANES
    vmem = pl.BlockSpec(memory_space=pltpu.VMEM)
    smem = pl.BlockSpec(memory_space=pltpu.SMEM)
    anywhere = pl.BlockSpec(memory_space=pl.ANY)
    dma = pltpu.SemaphoreType.DMA
    shape = jax.ShapeDtypeStruct
    span = min(PART_UNITS, half_width)
    parts = half_width // span
    pieces = parts * HALVES
    chunked = pltpu.VMEM((pieces, depth // HALVES, 3 * span), BF16)
    state_in, state_down = shape((depth, wide), BF16), shape((depth, half_width), BF16)
    moments = (m_in[0], m_down[0], v_in[0], v_down[0])
    total, weight, back, hots, *moved = pl.pallas_call(
        layer_kernel,
        name="layer",
        out_shape=(
            shape((depth, joint), F32),
            shape((depth, joint), BF16),
            shape((room, width + LANES), BF16),
            shape((top_count, tok_rows, room), BF16),
        )
        + (state_in, state_down) * 2,
        in_specs=[vmem, vmem, smem] + [vmem] * 5 + [anywhere] * 4,
        out_specs=(vmem,) * 4 + (anywhere,) * 4,
        scratch_shapes=[
            pltpu.VMEM((planes, tok_rows, row_width), BF16),
            pltpu.VMEM((room, row_width), BF16),
            pltpu.VMEM((room, row_width), BF16),
            pltpu.VMEM((parts, dp * depth, 3 * span), BF16),
            pltpu.VMEM((depth, wide), BF16),
            pltpu.VMEM((depth, half_width), BF16),
            pltpu.VMEM((room, width), BF16),
            pltpu.VMEM((width, room), BF16),
            pltpu.VMEM((width, room), BF16),
            pltpu.VMEM((parts, room, 2 * span), BF16),
            pltpu.VMEM((parts, room, span), BF16),
            pltpu.VMEM((parts, dp, depth, 3 * span), BF16),
        ]
        + [chunked] * 7
        + [dma((3, 2, 3))] * 2
        + [dma((experts,))] * 4
        + [dma((3, parts))] * 2
        + [dma((4,))] * 2
        + [dma((7, parts))] * 2
        + [dma((7, pieces))] * 2,
        compiler_params=pltpu.CompilerParams(
            collective_id=0, has_side_effects=True, vmem_limit_bytes=VMEM_BYTES
        ),
    )(
        expert_ids.T,
        held_expert.reshape(1, experts),
        swap_pairs,
        gate_probs.T,
        tokens,
        out_grad,
        w_in[0],
        w_down[0],
        *moments,
    )
    steps = ADAM_STEPS

    def rows(columns):
        return pl.BlockSpec((depth // steps, columns), lambda i: (i, 0))

    states = [rows(wide), rows(half_width)]
    result = pl.pallas_call(
        update_kernel,
        name="update",
        grid=(steps,),
        out_shape=(shape((tok_rows, width), BF16), shape((top_count, tok_rows), F32))
        + (state_in, state_down) * 3,
        in_specs=[
            smem,
            rows(joint),
            rows(joint),
            pl.BlockSpec((room, width // steps), lambda i: (0, i)),
            pl.BlockSpec((room, LANES), lambda i: (0, width // LANES)),
            pl.BlockSpec((top_count, tok_rows, room), lambda i: (0, 0, 0)),
        ]
        + states * 4,
        out_specs=[
            pl.BlockSpec((tok_rows, width // steps), lambda i: (0, i)),
            pl.BlockSpec((top_count, tok_rows), lambda i: (0, 0)),
        ]
        + states * 3,
    )(swap_pairs, total, weight, back, back, hots, *moments, *moved)
    return (result[0], result[1].T) + tuple(r[None] for r in result[2:])


def solution(mesh):
    experts = mesh.shape["expert"]
    shape = (2, 4, experts // 8, 4, 2)
    split = Mesh(mesh.devices.reshape(shape), DP_EXPERT)
    rows = P(DP_EXPERT, None)
    state = P(EXPERT, DP, None)
    return jax.shard_map(
        body,
        mesh=split,
        in_specs=(rows,) * 4 + (P(), P()) + (state,) * 6,
        out_specs=(rows, rows) + (state,) * 6,
        check_vma=False,
    )
```

```python
import functools

import jax
import jax.numpy as jnp
from jax import lax
from jax.experimental import pallas as pl
from jax.experimental.pallas import tpu as pltpu
from jax.sharding import Mesh
from jax.sharding import PartitionSpec as P

DP = ("dp_0", "dp_1")
EXPERT = ("ex", "ez", "ec")
DP_EXPERT = DP + EXPERT
MESH = pl.DeviceIdType.MESH
BF16, F32 = jnp.bfloat16, jnp.float32

beta_one = 0.9
beta_two = 0.95
learn_rate = 0.01
adam_eps = 1e-08
bias_one = 1.0 - 0.9**10
bias_two = 1.0 - 0.95**10

LANES = 128
PART_UNITS = 256
HALVES = 4
ADAM_STEPS = 4
VMEM_BYTES = 60 * 1024 * 1024


def in_parts(column):
    high = column.astype(BF16).astype(F32)
    rest = column - high
    middle = rest.astype(BF16).astype(F32)
    return [high, middle, rest - middle]


def in_lanes(columns):
    lane = lax.broadcasted_iota(jnp.int32, (columns[0].shape[0], LANES), 1)
    result = jnp.zeros(lane.shape, F32)
    for n, column in enumerate(columns):
        result = jnp.where(lane == n, column, result)
    return result.astype(BF16)


def from_parts(parts, start=0):
    parts = parts.astype(F32)
    high, middle, low = (parts[:, start + n : start + n + 1] for n in range(3))
    return high + middle + low


def column_of(row, turn=0):
    n = row.shape[1]
    at, lane = (lax.broadcasted_iota(jnp.int32, (n, n), d) for d in (0, 1))
    return jnp.sum(jnp.where(lane == lax.rem(at + turn, n), row, 0.0), axis=1, keepdims=True)


def row_of(column):
    n = column.shape[0]
    at, lane = (lax.broadcasted_iota(jnp.int32, (n, n), d) for d in (0, 1))
    return jnp.sum(jnp.where(lane == at, column, 0.0), axis=0, keepdims=True)


def dot(a, b, contract=(1, 0)):
    dims = (((contract[0],), (contract[1],)), ((), ()))
    return lax.dot_general(a, b, dims, preferred_element_type=F32)


def swapped_here(pairs_ref, me, half_axis):
    mine = lax.rem(me, half_axis)
    flag = (mine == pairs_ref[0]).astype(jnp.int32)
    for j in range(1, pairs_ref.shape[0]):
        flag = jnp.maximum(flag, (mine == pairs_ref[j]).astype(jnp.int32))
    return flag


def choose(flag, moved, kept):
    return jnp.where(jnp.full(kept.shape, flag, jnp.int32) > 0, moved.astype(F32), kept.astype(F32))


def send(source, target, sems, at, device):
    return pltpu.make_async_remote_copy(
        src_ref=source,
        dst_ref=target,
        send_sem=sems[0].at[at],
        recv_sem=sems[1].at[at],
        device_id=device,
        device_id_type=MESH,
    )


class Place:
    def __init__(self):
        self.z, self.y = lax.axis_index("dp_0"), lax.axis_index("dp_1")
        self.layers, self.ring = lax.axis_size("dp_0"), lax.axis_size("dp_1")
        self.cores, self.planes = lax.axis_size("ec"), lax.axis_size("ez")
        self.side = lax.axis_size("ex") * self.cores
        self.experts = self.side * self.planes
        self.own = lax.axis_index("ex") * self.cores + lax.axis_index("ec")
        self.plane = lax.axis_index("ez")
        self.me = (
            lax.axis_index("ex") * self.planes + self.plane
        ) * self.cores + lax.axis_index("ec")
        self.across = {"dp_0": 1 - self.z}
        self.up = {"dp_1": lax.rem(self.y + 1, self.ring)}
        self.down = {"dp_1": lax.rem(self.y + self.ring - 1, self.ring)}

    def member(self, sideways, planes):
        q = (self.own + sideways) % self.side
        z = (self.plane + planes) % self.planes
        return {"ex": q // self.cores, "ez": z, "ec": q % self.cores}

    def partner(self):
        e = (self.me + self.experts // 2) % self.experts
        return {
            "ex": e // (self.planes * self.cores),
            "ez": (e // self.cores) % self.planes,
            "ec": e % self.cores,
        }

    def offset(self, i):
        return (i % 2) * ((i + 1) // 2) + (1 - i % 2) * (self.experts - i // 2)

    def shard(self, layer, step):
        z = (self.z + layer) % self.layers
        return z * self.ring + (self.y + step) % self.ring

    def greet(self):
        barrier = pltpu.get_barrier_semaphore()

        def hello(k, carry):
            device = self.member(k % self.side, k // self.side)
            pl.semaphore_signal(barrier, inc=1, device_id=device, device_id_type=MESH)
            return carry

        lax.fori_loop(1, self.experts, hello, 0)
        for device in (self.across, self.up, self.down):
            pl.semaphore_signal(barrier, inc=1, device_id=device, device_id_type=MESH)
        pl.semaphore_wait(barrier, self.experts - 1 + 3)


def layer_kernel(
    ids_ref, held_ref, pairs_ref, probs_ref, tokens_ref, grads_ref, w_in_ref, w_down_ref,
    m_in_ref, m_down_ref, v_in_ref, v_down_ref,
    total_ref, weight_ref, back, hots_ref, pm_in, pm_down, pv_in, pv_down,
    tok, send_ref, recv, full_ref, swap_in, swap_down, scaled, x_turned, s_turned, pre, hidden, grad,
    on_up, on_down, a_low, a_high, b_low, b_high, z_in,
    tok_send, tok_recv, row_send, row_recv, back_send, back_recv, swap_send, swap_recv,
    moment_send, moment_recv, gather_send, gather_recv, ring_send, ring_recv,
):
    at = Place()
    experts, half_axis = at.experts, at.experts // 2
    tok_rows, width = tokens_ref.shape
    room, row_width = recv.shape
    capacity = room // experts
    plane_room = room // at.planes
    depth, wide = w_in_ref.shape
    half_width = w_down_ref.shape[1]
    at.greet()

    half_rows = tok_rows // 2
    tok_sems = (tok_send, tok_recv)
    plane_up, plane_down = at.member(0, 1), at.member(0, at.planes - 1)
    pieces = (pl.ds(0, width), pl.ds(width, width), pl.ds(2 * width, LANES))

    def block(d, h, piece):
        return tok.at[d, pl.ds(h * half_rows, half_rows), pieces[piece]]

    def to_plane(kind, h, piece):
        if kind == 2:
            source, device = (block(1, 0, piece), plane_up) if h == 0 else (block(3, 1, piece), plane_down)
            target = block(2, h, piece)
        else:
            rows = pl.ds(h * half_rows, half_rows)
            source = (tokens_ref.at[rows], grads_ref.at[rows], block(0, h, piece))[piece]
            target, device = (block(1, h, piece), plane_up) if kind == 0 else (block(3, h, piece), plane_down)
        return send(source, target, tok_sems, (kind, h, piece), device)

    for piece in range(2):
        to_plane(0, 0, piece).start()
        to_plane(1, 1, piece).start()

    span = min(PART_UNITS, half_width)
    parts = half_width // span
    partner = at.partner()
    sems = (swap_send, swap_recv)
    swaps = []
    for c in range(parts):
        gate, up = pl.ds(c * span, span), pl.ds(half_width + c * span, span)
        swaps.append(
            (
                send(w_in_ref.at[:, gate], swap_in.at[:, gate], sems, (0, c), partner),
                send(w_in_ref.at[:, up], swap_in.at[:, up], sems, (1, c), partner),
                send(w_down_ref.at[:, gate], swap_down.at[:, gate], sems, (2, c), partner),
            )
        )
        for copy in swaps[-1]:
            copy.start()

    slot = lax.broadcasted_iota(jnp.int32, (1, experts), 1)
    flag = (lax.rem(slot, half_axis) == pairs_ref[0]).astype(jnp.int32)
    for j in range(1, pairs_ref.shape[0]):
        flag = jnp.maximum(flag, (lax.rem(slot, half_axis) == pairs_ref[j]).astype(jnp.int32))
    before_swap = held_ref[...].astype(F32)
    held = jnp.where(flag > 0, row_of(column_of(before_swap, half_axis)), before_swap)
    top_count = ids_ref.shape[0]
    hits = [
        (column_of(ids_ref[k : k + 1, :].astype(F32)) == held).astype(F32)
        for k in range(top_count)
    ]
    named = hits[0]
    for hit in hits[1:]:
        named = named + hit
    row, column = (lax.broadcasted_iota(jnp.int32, (tok_rows, tok_rows), d) for d in (0, 1))
    before = dot((column < row).astype(F32).astype(BF16), named.astype(BF16))
    in_plane = lax.div(slot, at.planes * at.cores) * at.cores + lax.rem(slot, at.cores)
    planes_on = lax.rem(lax.rem(lax.div(slot, at.cores), at.planes) + at.planes - at.plane, at.planes)
    sideways = lax.rem(in_plane + at.side - at.own, at.side)
    first = ((planes_on * at.side + sideways) * capacity).astype(F32)
    room_ids = lax.broadcasted_iota(jnp.int32, (tok_rows, room), 1)
    columns = []
    for k in range(top_count):
        columns += in_parts(column_of(probs_ref[k : k + 1, :]))
    for k, hit in enumerate(hits):
        place = jnp.sum(hit * (before + first), axis=1, keepdims=True).astype(jnp.int32)
        hots_ref[k] = (room_ids == place).astype(F32).astype(BF16)
        high = lax.div(place, capacity)
        columns += [high.astype(F32), (place - high * capacity).astype(F32)]
    tok[0, :, pl.ds(2 * width, LANES)] = in_lanes(columns)
    to_plane(0, 0, 2).start()
    to_plane(1, 1, 2).start()

    def row_copy(d, r):
        rows = pl.ds(pl.multiple_of(d * plane_room + r * capacity, capacity), capacity)
        n = d * at.side + r
        return send(
            send_ref.at[rows], recv.at[rows], (row_send, row_recv), n, at.member(r, 0)
        )

    def dispatch(d):
        lanes = tok[d, :, pl.ds(2 * width, LANES)]
        slots = lax.broadcasted_iota(jnp.int32, (tok_rows, plane_room), 1) + d * plane_room
        lane = lax.broadcasted_iota(jnp.int32, lanes.shape, 1)
        number = lanes.astype(F32)
        both = jnp.zeros((plane_room, tok_rows), F32)
        values = jnp.zeros((plane_room, LANES), F32)
        for k in range(top_count):
            start = 3 * top_count + 2 * k
            place = number[:, start : start + 1] * capacity + number[:, start + 1 : start + 2]
            hot = (slots == place.astype(jnp.int32)).astype(F32).T
            both = both + hot
            own = jnp.where(lane >= 3 * k, jnp.where(lane < 3 * k + 3, number, 0.0), 0.0)
            values = values + dot(hot.astype(BF16), own.astype(BF16))
        rows = pl.ds(d * plane_room, plane_room)
        both = both.astype(BF16)
        step = min(512, width)
        for c in range(2 * width // step):
            columns = pl.ds(c * step, step)
            if d > 0:
                source = tok[d, :, columns]
            elif c * step < width:
                source = tokens_ref[:, columns]
            else:
                source = grads_ref[:, pl.ds(c * step - width, step)]
            send_ref[rows, columns] = dot(both, source).astype(BF16)
        send_ref[rows, pl.ds(2 * width, LANES)] = values.astype(BF16)

        def start_row(r, carry):
            row_copy(d, r).start()
            return carry

        lax.fori_loop(1, at.side, start_row, 0)
        own_rows = pl.ds(d * plane_room, capacity)
        recv[own_rows] = send_ref[own_rows]

    def take_rows(d):
        def wait_row(r, carry):
            row_copy(d, r).wait_recv()
            return carry

        lax.fori_loop(1, at.side, wait_row, 0)
        rows = pl.ds(d * plane_room, plane_room)
        lanes = recv[rows, pl.ds(2 * width, LANES)]
        rows_p = from_parts(lanes)
        for k in range(1, top_count):
            rows_p = rows_p + from_parts(lanes, 3 * k)
        step = min(512, width)
        for c in range(width // step):
            columns = pl.ds(c * step, step)
            rows_g = recv[rows, pl.ds(width + c * step, step)].astype(F32)
            rows_s = (rows_p * rows_g).astype(BF16)
            scaled[rows, columns] = rows_s
            s_turned[columns, rows] = rows_s.T
            x_turned[columns, rows] = recv[rows, columns].T

    dispatch(0)

    flag = swapped_here(pairs_ref, at.me, half_axis)
    gather = (gather_send, gather_recv)

    def shard(layer, step, c):
        start = at.shard(layer, step) * depth
        return full_ref.at[c, pl.ds(pl.multiple_of(start, depth), depth)]

    def spread(kind, layer, step, c, device):
        shared = shard(layer, step, c)
        return send(shared, shared, gather, (kind, c), device)

    spreading = []

    def begin_spread(*what):
        copy = spread(*what)
        copy.start()
        spreading.append(copy)

    ACROSS, UP_OWN, DOWN_OWN, UP_OTHER, DOWN_OTHER, UP_ON, DOWN_ON = range(7)

    def open_gather(c):
        for copy in swaps[c]:
            copy.wait_recv()
        mine = shard(0, 0, c)
        for n, (here, there, start) in enumerate(
            ((w_in_ref, swap_in, 0), (w_in_ref, swap_in, half_width), (w_down_ref, swap_down, 0))
        ):
            columns = pl.ds(start + c * span, span)
            new = choose(flag, there[:, columns], here[:, columns]).astype(BF16)
            mine[:, pl.ds(n * span, span)] = new
            weight_ref[:, pl.ds(n * half_width + c * span, span)] = new
        begin_spread(UP_OWN, 0, 0, c, at.up)
        begin_spread(DOWN_OWN, 0, 0, c, at.down)

    def cross(c):
        begin_spread(ACROSS, 0, 0, c, at.across)

    def pass_own(c):
        spread(UP_OWN, 0, -1, c, at.up).wait_recv()
        begin_spread(UP_ON, 0, -1, c, at.up)

    def spread_other(c):
        spread(ACROSS, 1, 0, c, at.across).wait_recv()
        begin_spread(UP_OTHER, 1, 0, c, at.up)
        begin_spread(DOWN_OTHER, 1, 0, c, at.down)

    def pass_other(c):
        spread(DOWN_OTHER, 1, 1, c, at.down).wait_recv()
        begin_spread(DOWN_ON, 1, 1, c, at.down)

    every = range(parts)

    def more_blocks():
        for piece in range(3):
            to_plane(0, 1, piece).start()
            to_plane(1, 0, piece).start()

    def pass_blocks():
        for kind, h in ((0, 0), (1, 1)):
            for piece in range(3):
                to_plane(kind, h, piece).wait_recv()
            for piece in range(3):
                to_plane(2, h, piece).start()

    def spread_block(d):
        for kind, h in {1: ((0, 1),), 3: ((1, 0),), 2: ((2, 0), (2, 1))}[d]:
            for piece in range(3):
                to_plane(kind, h, piece).wait_recv()
        dispatch(d)

    pairs_of = ((m_in_ref, pm_in), (m_down_ref, pm_down), (v_in_ref, pv_in), (v_down_ref, pv_down))
    moments = [
        send(own, other, (moment_send, moment_recv), n, partner)
        for n, (own, other) in enumerate(pairs_of)
    ]
    for c in every:
        open_gather(c)
        cross(c)
    more_blocks()
    for c in every[:-1]:
        pass_own(c)
    pass_blocks()
    for c in every[:-1]:
        spread_other(c)
    pass_own(parts - 1)
    spread_other(parts - 1)
    spread_block(1)
    pass_other(0)
    spread_block(3)
    for c in every[1:]:
        pass_other(c)
    spread_block(2)
    for copy in moments[:2]:
        copy.start()

    def gathered(c):
        spread(DOWN_OWN, 0, 1, c, at.down).wait_recv()
        spread(UP_OTHER, 1, -1, c, at.up).wait_recv()
        spread(UP_ON, 0, -2, c, at.up).wait_recv()
        spread(DOWN_ON, 1, 2, c, at.down).wait_recv()

    for d in (0, 1, 3):
        take_rows(d)
    gathered(0)
    take_rows(2)

    ring = (ring_send, ring_recv)
    summing = []
    part = depth // HALVES

    def begin(source, target, kind, c, device):
        copy = send(source, target.at[c], ring, (kind, c), device)
        copy.start()
        summing.append(copy)

    def arrived(target, kind, c):
        send(target.at[c], target.at[c], ring, (kind, c), at.up).wait_recv()
        return target[c].astype(F32)

    def piece_of(i, c):
        return grad.at[c // HALVES, i, pl.ds((c % HALVES) * part, part)]

    A2, B2, A3, B3, A0, B0, A1, B1 = range(8)
    ON_UP, ON_DOWN, A_LOW, A_HIGH, B_LOW, B_HIGH, Z = range(7)

    def through(n):
        gate_part = dot(recv[:, :width], full_ref[n, :, pl.ds(0, span)])
        up_part = dot(recv[:, :width], full_ref[n, :, pl.ds(span, span)])
        hidden_grad = dot(scaled[...], full_ref[n, :, pl.ds(2 * span, span)])
        sigmoid = jax.nn.sigmoid(gate_part)
        activated = gate_part * sigmoid
        slope_term = sigmoid * (1.0 + gate_part * (1.0 - sigmoid))
        hidden[n] = (activated * up_part).astype(BF16)
        pre[n, :, pl.ds(0, span)] = (hidden_grad * up_part * slope_term).astype(BF16)
        pre[n, :, pl.ds(span, span)] = (hidden_grad * activated).astype(BF16)

    def sum_up(n):
        def weight_grads(i, carry):
            start = pl.multiple_of(at.shard(i % 2, 2 + i // 2) * depth, depth)
            rows = pl.ds(start, depth)
            grad[n, i, :, pl.ds(0, 2 * span)] = dot(x_turned[rows], pre[n]).astype(BF16)
            grad[n, i, :, pl.ds(2 * span, span)] = dot(s_turned[rows], hidden[n]).astype(BF16)
            return carry

        pieces_here = range(n * HALVES, (n + 1) * HALVES)
        lax.fori_loop(0, 2, weight_grads, 0)
        for c in pieces_here:
            begin(piece_of(A2, c), on_up, ON_UP, c, at.up)
            begin(piece_of(B2, c), on_down, ON_DOWN, c, at.down)
        lax.fori_loop(2, 8, weight_grads, 0)
        for c in pieces_here:
            begin(piece_of(B1, c), b_low, B_LOW, c, at.up)
            begin(piece_of(A3, c), a_high, A_HIGH, c, at.down)

    for n in every:
        if n > 0:
            gathered(n)
        through(n)
        if n == 0:
            sum_up(n)

    def wait_sent(d, carry):
        def wait_row(r, carry):
            row_copy(d, r).wait_send()
            return carry

        return lax.fori_loop(1, at.side, wait_row, carry)

    lax.fori_loop(0, at.planes, wait_sent, 0)

    span_out = min(256, width)

    ret = send_ref

    def row_grads(i, total):
        start = pl.multiple_of(i * span_out, span_out)
        rows = pl.ds(start, span_out)
        row_grad = jnp.zeros((room, span_out), F32)
        out = jnp.zeros((room, span_out), F32)
        for n in every:
            row_grad = row_grad + dot(pre[n], full_ref[n, rows, pl.ds(0, 2 * span)], (1, 1))
            out = out + dot(hidden[n], full_ref[n, rows, pl.ds(2 * span, span)], (1, 1))
        ret[:, rows] = row_grad.astype(BF16)
        rows_g = recv[:, pl.ds(pl.multiple_of(width + start, span_out), span_out)].astype(F32)
        return total + jnp.sum(out.astype(BF16).astype(F32) * rows_g, axis=1, keepdims=True)

    row_total = lax.fori_loop(0, width // span_out, row_grads, jnp.zeros((room, 1), F32))
    ret[:, pl.ds(width, LANES)] = in_lanes(in_parts(row_total))

    def rows_to(i):
        k = at.offset(i)
        rows = pl.ds(pl.multiple_of(k * capacity, capacity), capacity)
        device = at.member(at.side - k % at.side, at.planes - k // at.side)
        source = ret.at[rows, pl.ds(0, width + LANES)]
        return send(source, back.at[rows], (back_send, back_recv), k, device)

    def start_rows(i, carry):
        rows_to(i).start()
        return carry

    def wait_rows(i, carry):
        rows_to(i).wait()
        return carry

    lax.fori_loop(1, experts, start_rows, 0)
    for copy in moments[2:]:
        copy.start()
    back[0:capacity] = ret[0:capacity, pl.ds(0, width + LANES)]

    for n in every[1:]:
        sum_up(n)

    def pass_on(c):
        low, high = piece_of(A1, c), piece_of(B3, c)
        low[...] = (low[...].astype(F32) + arrived(on_up, ON_UP, c)).astype(BF16)
        begin(low, a_low, A_LOW, c, at.up)
        high[...] = (high[...].astype(F32) + arrived(on_down, ON_DOWN, c)).astype(BF16)
        begin(high, b_high, B_HIGH, c, at.down)

    def hand_over(c):
        other = piece_of(B0, c)
        mine = other[...].astype(F32) + arrived(b_low, B_LOW, c) + arrived(b_high, B_HIGH, c)
        other[...] = mine.astype(BF16)
        begin(other, z_in, Z, c, at.across)

    def add_up(c):
        mine = piece_of(A0, c)[...].astype(F32)
        mine = mine + arrived(a_low, A_LOW, c) + arrived(a_high, A_HIGH, c)
        mine = mine + arrived(z_in, Z, c)
        rows = pl.ds((c % HALVES) * part, part)
        for n in range(3):
            columns = pl.ds(n * half_width + c // HALVES * span, span)
            total_ref[rows, columns] = mine[:, n * span : (n + 1) * span]

    count = parts * HALVES
    for c in range(count):
        pass_on(c)
    for c in range(count):
        hand_over(c)
        if c > 0:
            add_up(c - 1)
    add_up(count - 1)
    lax.fori_loop(1, experts, wait_rows, 0)
    for copy in moments:
        copy.wait()

    for kind in range(3):
        for h in range(2):
            for piece in range(3):
                to_plane(kind, h, piece).wait_send()
    for pair in swaps:
        for copy in pair:
            copy.wait_send()
    for copy in spreading + summing:
        copy.wait_send()


def update_kernel(
    pairs_ref, total_ref, weight_ref, back, back_lanes, hots_ref,
    m_in_ref, m_down_ref, v_in_ref, v_down_ref, pm_in, pm_down, pv_in, pv_down,
    token_ref, prob_ref, nw_in, nw_down, nm_in, nm_down, nv_in, nv_down,
):
    at = Place()
    flag = swapped_here(pairs_ref, at.me, at.experts // 2)
    wide, half_width = m_in_ref.shape[1], m_down_ref.shape[1]
    for start, size, refs in (
        (0, wide, (pm_in, m_in_ref, pv_in, v_in_ref, nw_in, nm_in, nv_in)),
        (wide, half_width, (pm_down, m_down_ref, pv_down, v_down_ref, nw_down, nm_down, nv_down)),
    ):
        columns = pl.ds(start, size)
        value = total_ref[:, columns]
        first = choose(flag, refs[0][...], refs[1][...])
        second = choose(flag, refs[2][...], refs[3][...])
        weight = weight_ref[:, columns].astype(F32)
        first_new = beta_one * first + (1.0 - beta_one) * value
        second_new = beta_two * second + (1.0 - beta_two) * value * value
        root = jnp.sqrt(second_new * (1.0 / bias_two)) + adam_eps
        step_size = first_new * (1.0 / bias_one) / root
        refs[4][...] = (weight - learn_rate * step_size).astype(BF16)
        refs[5][...] = first_new.astype(BF16)
        refs[6][...] = second_new.astype(BF16)
    hots = [hots_ref[k] for k in range(hots_ref.shape[0])]
    both = hots[0]
    for hot in hots[1:]:
        both = both + hot
    token_ref[...] = dot(both, back[...]).astype(BF16)

    @pl.when(pl.program_id(0) == 0)
    def _():
        for k, hot in enumerate(hots):
            prob_ref[k : k + 1, :] = row_of(from_parts(dot(hot, back_lanes[...])))


def body(
    tokens,
    out_grad,
    expert_ids,
    gate_probs,
    held_expert,
    swap_pairs,
    w_in,
    w_down,
    m_in,
    m_down,
    v_in,
    v_down,
):
    experts = lax.axis_size(EXPERT)
    planes, side = lax.axis_size("ez"), experts // lax.axis_size("ez")
    dp = lax.axis_size(DP)
    tok_rows, width = tokens.shape
    top_count = expert_ids.shape[1]
    capacity = max(2, 2 * tok_rows * top_count // experts)
    room = experts * capacity
    _, depth, wide = w_in.shape
    half_width = w_down.shape[2]
    joint = wide + half_width
    row_width = 2 * width + LANES
    vmem = pl.BlockSpec(memory_space=pltpu.VMEM)
    smem = pl.BlockSpec(memory_space=pltpu.SMEM)
    anywhere = pl.BlockSpec(memory_space=pl.ANY)
    dma = pltpu.SemaphoreType.DMA
    shape = jax.ShapeDtypeStruct
    span = min(PART_UNITS, half_width)
    parts = half_width // span
    pieces = parts * HALVES
    chunked = pltpu.VMEM((pieces, depth // HALVES, 3 * span), BF16)
    state_in, state_down = shape((depth, wide), BF16), shape((depth, half_width), BF16)
    moments = (m_in[0], m_down[0], v_in[0], v_down[0])
    total, weight, back, hots, *moved = pl.pallas_call(
        layer_kernel,
        name="layer",
        out_shape=(
            shape((depth, joint), F32),
            shape((depth, joint), BF16),
            shape((room, width + LANES), BF16),
            shape((top_count, tok_rows, room), BF16),
        )
        + (state_in, state_down) * 2,
        in_specs=[vmem, vmem, smem] + [vmem] * 5 + [anywhere] * 4,
        out_specs=(vmem,) * 4 + (anywhere,) * 4,
        scratch_shapes=[
            pltpu.VMEM((planes, tok_rows, row_width), BF16),
            pltpu.VMEM((room, row_width), BF16),
            pltpu.VMEM((room, row_width), BF16),
            pltpu.VMEM((parts, dp * depth, 3 * span), BF16),
            pltpu.VMEM((depth, wide), BF16),
            pltpu.VMEM((depth, half_width), BF16),
            pltpu.VMEM((room, width), BF16),
            pltpu.VMEM((width, room), BF16),
            pltpu.VMEM((width, room), BF16),
            pltpu.VMEM((parts, room, 2 * span), BF16),
            pltpu.VMEM((parts, room, span), BF16),
            pltpu.VMEM((parts, dp, depth, 3 * span), BF16),
        ]
        + [chunked] * 7
        + [dma((3, 2, 3))] * 2
        + [dma((experts,))] * 4
        + [dma((3, parts))] * 2
        + [dma((4,))] * 2
        + [dma((7, parts))] * 2
        + [dma((7, pieces))] * 2,
        compiler_params=pltpu.CompilerParams(
            collective_id=0, has_side_effects=True, vmem_limit_bytes=VMEM_BYTES
        ),
    )(
        expert_ids.T,
        held_expert.reshape(1, experts),
        swap_pairs,
        gate_probs.T,
        tokens,
        out_grad,
        w_in[0],
        w_down[0],
        *moments,
    )
    steps = ADAM_STEPS

    def rows(columns):
        return pl.BlockSpec((depth // steps, columns), lambda i: (i, 0))

    states = [rows(wide), rows(half_width)]
    result = pl.pallas_call(
        update_kernel,
        name="update",
        grid=(steps,),
        out_shape=(shape((tok_rows, width), BF16), shape((top_count, tok_rows), F32))
        + (state_in, state_down) * 3,
        in_specs=[
            smem,
            rows(joint),
            rows(joint),
            pl.BlockSpec((room, width // steps), lambda i: (0, i)),
            pl.BlockSpec((room, LANES), lambda i: (0, width // LANES)),
            pl.BlockSpec((top_count, tok_rows, room), lambda i: (0, 0, 0)),
        ]
        + states * 4,
        out_specs=[
            pl.BlockSpec((tok_rows, width // steps), lambda i: (0, i)),
            pl.BlockSpec((top_count, tok_rows), lambda i: (0, 0)),
        ]
        + states * 3,
    )(swap_pairs, total, weight, back, back, hots, *moments, *moved)
    return (result[0], result[1].T) + tuple(r[None] for r in result[2:])


def solution(mesh):
    experts = mesh.shape["expert"]
    shape = (2, 4, experts // 8, 4, 2)
    split = Mesh(mesh.devices.reshape(shape), DP_EXPERT)
    rows = P(DP_EXPERT, None)
    state = P(EXPERT, DP, None)
    return jax.shard_map(
        body,
        mesh=split,
        in_specs=(rows,) * 4 + (P(), P()) + (state,) * 6,
        out_specs=(rows, rows) + (state,) * 6,
        check_vma=False,
    )
```
